32 devices in a mesh: dp: 2 (over x), ff: 4 (over z), hd: 4 (over y, core).
Axes of the slice: x: 2, y: 2, z: 4, core: 2. Of those that a mesh axis runs over, the one named last changes fastest.
Arguments:
- x_in: bfloat16 [256, 4096], P('dp', 'hd'), parts along dimension 0
- w_up: bfloat16 [4096, 20480], P('hd', 'ff')
- b_up: float32 [20480], P('ff')
- w_down: bfloat16 [10240, 4096], P('ff', 'hd')
- b_down: float32 [4096], P('hd')
- ln_gain: float32 [4096], P('hd')
- ln_bias: float32 [4096], P('hd')
- dy_in: bfloat16 [256, 4096], P('dp', 'hd'), parts along dimension 0
Outputs:
- output 1: bfloat16 [256, 4096], P('dp', 'hd'), parts along dimension 0
- output 2: bfloat16 [256, 4096], P('dp', 'hd'), parts along dimension 0
- output 3: float32 [8192, 20480], P(('dp', 'hd'), 'ff'), parts along dimension 0
- output 4: float32 [20480, 4096], P(('dp', 'ff'), 'hd'), parts along dimension 0
- output 5: float32 [40960], P(('dp', 'ff')), parts along dimension 0
- output 6: float32 [8192], P(('dp', 'hd')), parts along dimension 0
- output 7: float32 [8192], P(('dp', 'hd')), parts along dimension 0
- output 8: float32 [8192], P(('dp', 'hd')), parts along dimension 0
There are 2 independent parts. The reference program is written for one: setup_inputs(seed, part) draws one part's arguments, and reference() takes and returns one part's arrays. A program takes and returns all parts, laid end to end along the dimension named above; an argument that names none is the same for every part.
All inputs are finite; a program needn't handle non-finite values.
Results may differ from the reference program's by a relative error of at most 0.01878.
Values are sent between devices in bfloat16 or wider.
A program may use at most 1 GiB of HBM per device.

```python
import math
import jax
import jax.numpy as jnp
from jax import lax

TOKENS = 128
HIDDEN = 4096
FFN = 10240
PAIR = 128
COARSE = 16
ALPHA = math.sqrt(140.0)
LN_EPS = 1e-5


def setup_inputs(seed: int = 0, part: int = 0) -> dict:
    part_keys = jax.random.split(jax.random.fold_in(jax.random.key(seed), part), 7)
    shared_keys = jax.random.split(jax.random.key(seed + 1), 6)
    seg_width = HIDDEN // COARSE
    row_shift = 0.7 * jax.random.normal(part_keys[0], (TOKENS, 1, 1), jnp.float32)
    seg_shift = 0.8 * jax.random.normal(part_keys[1], (1, COARSE, 1), jnp.float32)
    seg_scale = jnp.exp(0.4 * jax.random.normal(part_keys[2], (1, COARSE, 1), jnp.float32))
    x_noise = jax.random.normal(part_keys[3], (TOKENS, COARSE, seg_width), jnp.float32)
    x_vals = (row_shift + seg_shift + seg_scale * x_noise).reshape(TOKENS, HIDDEN)
    dy_noise = jax.random.normal(part_keys[4], (TOKENS, COARSE, seg_width), jnp.float32)
    dy_shift = 0.8 * jax.random.normal(part_keys[5], (TOKENS, 1, 1), jnp.float32)
    dy_tilt = jax.random.normal(part_keys[6], (TOKENS, 1, 1), jnp.float32)
    dy_vals = (dy_noise + dy_shift + dy_tilt * seg_shift).reshape(TOKENS, HIDDEN)
    w_up = jax.random.normal(shared_keys[0], (HIDDEN, 2 * FFN), jnp.float32) * HIDDEN ** -0.5
    b_up = 0.5 * jax.random.normal(shared_keys[1], (2 * FFN,), jnp.float32)
    w_down = jax.random.normal(shared_keys[2], (FFN, HIDDEN), jnp.float32) * (ALPHA * FFN ** -0.5)
    b_down = 3.0 * jax.random.normal(shared_keys[3], (HIDDEN,), jnp.float32)
    ln_gain = 1.0 + 0.3 * jax.random.normal(shared_keys[4], (HIDDEN,), jnp.float32)
    ln_bias = 0.3 * jax.random.normal(shared_keys[5], (HIDDEN,), jnp.float32)
    return {'x_in': x_vals.astype(jnp.bfloat16), 'w_up': w_up.astype(jnp.bfloat16), 'b_up': b_up, 'w_down': w_down.astype(jnp.bfloat16), 'b_down': b_down, 'ln_gain': ln_gain, 'ln_bias': ln_bias, 'dy_in': dy_vals.astype(jnp.bfloat16)}


def gelu_tanh(z_val):
    return jax.nn.gelu(z_val, approximate=True)


def reference(x_in, w_up, b_up, w_down, b_down, ln_gain, ln_bias, dy_in):
    n_blocks = FFN // PAIR
    u_acc = jnp.dot(x_in, w_up, preferred_element_type=jnp.float32) + b_up
    u_act = u_acc.astype(jnp.bfloat16).reshape(TOKENS, n_blocks, 2, PAIR)
    val_half = u_act[:, :, 0, :].astype(jnp.float32)
    gate_half = u_act[:, :, 1, :].astype(jnp.float32)
    gelu_out, gelu_vjp = jax.vjp(gelu_tanh, gate_half)
    m_act = (val_half * gelu_out).astype(jnp.bfloat16).reshape(TOKENS, FFN)
    f_out = jnp.dot(m_act, w_down, preferred_element_type=jnp.float32)
    residual = ALPHA * x_in.astype(jnp.float32) + f_out + b_down
    row_mean = jnp.mean(residual, axis=1, keepdims=True)
    centered = residual - row_mean
    row_var = jnp.mean(centered * centered, axis=1, keepdims=True)
    inv_std = lax.rsqrt(row_var + LN_EPS)
    normed = centered * inv_std
    y_out = (ln_gain * normed + ln_bias).astype(jnp.bfloat16)
    dy_f = dy_in.astype(jnp.float32)
    g_dy = dy_f * ln_gain
    d_resid = inv_std * (g_dy - jnp.mean(g_dy, axis=1, keepdims=True) - normed * jnp.mean(g_dy * normed, axis=1, keepdims=True))
    dr_b = d_resid.astype(jnp.bfloat16)
    d_mact = jnp.dot(dr_b, w_down.T, preferred_element_type=jnp.float32).reshape(TOKENS, n_blocks, PAIR)
    d_val = d_mact * gelu_out
    d_gate = gelu_vjp(d_mact * val_half)[0]
    du_f = jnp.stack([d_val, d_gate], axis=2).reshape(TOKENS, 2 * FFN)
    du_b = du_f.astype(jnp.bfloat16)
    dw_up = jnp.dot(x_in.T, du_b, preferred_element_type=jnp.float32)
    dw_down = jnp.dot(m_act.T, dr_b, preferred_element_type=jnp.float32)
    dx_out = (ALPHA * d_resid + jnp.dot(du_b, w_up.T, preferred_element_type=jnp.float32)).astype(jnp.bfloat16)
    return (y_out, dx_out, dw_up, dw_down, jnp.sum(du_f, axis=0), jnp.sum(d_resid, axis=0), jnp.sum(dy_f * normed, axis=0), jnp.sum(dy_f, axis=0))
```

```python
import functools
import math

import jax
import jax.numpy as jnp
from jax import lax
from jax.experimental import pallas as pl
from jax.experimental.pallas import tpu as pltpu
from jax.sharding import PartitionSpec as P

PAIR = 128
ALPHA = math.sqrt(140.0)
LN_EPS = 1e-5
GELU_K = math.sqrt(2.0 / math.pi)
GELU_C = 0.044715
MESH = pl.DeviceIdType.MESH
F32 = jnp.float32
BF16 = jnp.bfloat16

GROUPS = 1
LOOKAHEAD = 3


def gelu_parts(z):
    t = jnp.tanh(GELU_K * (z + GELU_C * (z * z * z)))
    cdf = 0.5 * (1.0 + t)
    slope = cdf + z * (0.5 * (1.0 - t * t) * (GELU_K * (1.0 + (3.0 * GELU_C) * (z * z))))
    return z * cdf, slope


def dot_nt(a, b):
    return lax.dot_general(a, b, (((1,), (1,)), ((), ())), preferred_element_type=F32)


def dot_tn(a, b):
    return lax.dot_general(a, b, (((0,), (0,)), ((), ())), preferred_element_type=F32)


def main_kernel(
    x_ref, w1_hbm, b1_ref, w2_hbm, b2_ref, gam_ref, bet_ref, dy_ref,
    y_ref, m_ref, d_ref, du_ref, dx0_ref, dx1_ref, dx2_ref, dx3_ref, drz_ref, db1_ref, db2_ref, dgam_ref, dbet_ref,
    w1b, w2b, upart, uhalf, usend, uin, ubuf, mbuf, facc, zsend, zin, fsum, stat_in, tmp, dr_buf,
    npart, nhalf, nsend, nin, nbuf, dxacc,
    wsem, chunk_s, chunk_r, full_s, full_r, zsem_s, zsem_r, stat_s, stat_r,
):
    n_ch = w1b.shape[0]
    hid = x_ref.shape[1]
    tokens = x_ref.shape[0]
    hidden = 4 * hid
    tn = tokens // GROUPS
    rz = tn // 4
    cw = 8 * PAIR
    q = lax.axis_index('hd')
    z = lax.axis_index('ff')
    k = lax.rem(q, 2)
    y = lax.div(q, 2)
    pq = q + 1 - 2 * k
    yq = lax.rem(q + 2, 4)
    dq = lax.rem(pq + 2, 4)

    def remote(src, dst, ss, rs, **dev):
        return pltpu.make_async_remote_copy(src_ref=src, dst_ref=dst, send_sem=ss, recv_sem=rs, device_id=dev, device_id_type=MESH)

    w_copies = [pltpu.make_async_copy(w1_hbm.at[:, pl.ds(cw * c, cw)], w1b.at[c], wsem.at[c]) for c in range(n_ch)]
    w_copies += [pltpu.make_async_copy(w2_hbm.at[pl.ds(4 * PAIR * c, 4 * PAIR), :], w2b.at[c], wsem.at[n_ch + c]) for c in range(n_ch)]
    started = [0]

    def need_weight(i):
        while started[0] < min(i + LOOKAHEAD, 2 * n_ch):
            w_copies[started[0]].start()
            started[0] += 1

    need_weight(0)
    bar = pltpu.get_barrier_semaphore()
    for dz in range(4):
        for dh in range(4):
            if dz or dh:
                pl.semaphore_signal(bar, inc=1, device_id={'hd': lax.rem(q + dh, 4), 'ff': lax.rem(z + dz, 4)}, device_id_type=MESH)

    waits = []

    def make_group(g):
        row0 = g * tn
        rows = pl.ds(row0, tn)
        def ch(kind, c):
            return chunk_s.at[g, kind, c], chunk_r.at[g, kind, c]

        u_d2d = [remote(upart.at[g, c, 1 - k], uhalf.at[g, c], *ch(0, c), hd=pq) for c in range(n_ch)]
        u_y = [remote(usend.at[g, c], uin.at[g, c], *ch(1, c), hd=yq) for c in range(n_ch)]
        m_p = [remote(mbuf.at[g, c, q], mbuf.at[g, c, q], *ch(2, c), hd=pq) for c in range(n_ch)]
        m_y = [remote(mbuf.at[g, c, q], mbuf.at[g, c, q], *ch(3, c), hd=yq) for c in range(n_ch)]
        m_f = [remote(mbuf.at[g, c, yq], mbuf.at[g, c, yq], *ch(4, c), hd=pq) for c in range(n_ch)]
        n_d2d = [remote(npart.at[g, c, 1 - k], nhalf.at[g, c], *ch(5, c), hd=pq) for c in range(n_ch)]
        n_y = [remote(nsend.at[g, c], nin.at[g, c], *ch(6, c), hd=yq) for c in range(n_ch)]
        n_p = [remote(nbuf.at[g, c, q], nbuf.at[g, c, q], *ch(7, c), hd=pq) for c in range(n_ch)]
        n_yy = [remote(nbuf.at[g, c, q], nbuf.at[g, c, q], *ch(8, c), hd=yq) for c in range(n_ch)]
        n_f = [remote(nbuf.at[g, c, yq], nbuf.at[g, c, yq], *ch(9, c), hd=pq) for c in range(n_ch)]
        u_p = remote(ubuf.at[g, q], ubuf.at[g, q], full_s.at[g, 0], full_r.at[g, 0], hd=pq)
        u_yy = remote(ubuf.at[g, q], ubuf.at[g, q], full_s.at[g, 1], full_r.at[g, 1], hd=yq)
        u_f = remote(ubuf.at[g, yq], ubuf.at[g, yq], full_s.at[g, 2], full_r.at[g, 2], hd=pq)
        z_rs = [remote(zsend.at[g, lax.rem(z + d, 4)], zin.at[g, d - 1], zsem_s.at[g, 0, d - 1], zsem_r.at[g, 0, d - 1], ff=lax.rem(z + d, 4)) for d in range(1, 4)]
        z_ag = [remote(fsum.at[g, z], fsum.at[g, z], zsem_s.at[g, 1, d - 1], zsem_r.at[g, 1, d - 1], ff=lax.rem(z + d, 4)) for d in range(1, 4)]
        st = []
        for dz in range(4):
            for dh in range(4):
                if dz or dh:
                    i = dz * 4 + dh - 1
                    st.append(remote(stat_in.at[g, z, q], stat_in.at[g, z, q], stat_s.at[g, i], stat_r.at[g, i], hd=lax.rem(q + dh, 4), ff=lax.rem(z + dz, 4)))
        waits.extend(u_d2d + u_y + m_p + m_y + m_f + n_d2d + n_y + n_p + n_yy + n_f + [u_p, u_yy, u_f] + z_rs + z_ag + st)

        def s1(c):
            if g == 0:
                need_weight(c)
                w_copies[c].wait()
            for j in range(4):
                o = jnp.dot(x_ref[rows, :], w1b[c, :, 2 * PAIR * j:2 * PAIR * (j + 1)], preferred_element_type=F32)
                upart[g, c, j % 2, j // 2] = o.astype(BF16)
            if g == 0 and c == 0:
                pl.semaphore_wait(bar, 15)
            u_d2d[c].start()

        def s2(c):
            u_d2d[c].wait_recv()
            usend[g, c] = (upart[g, c, k, 1 - y].astype(F32) + uhalf[g, c, 1 - y].astype(F32)).astype(BF16)
            u_y[c].start()

        def s3(c):
            u_y[c].wait_recv()
            u = upart[g, c, k, y].astype(F32) + uhalf[g, c, y].astype(F32) + uin[g, c].astype(F32)
            u = (u + b1_ref[4 * c + q]).astype(BF16)
            ubuf[g, q, c] = u
            u = u.astype(F32)
            gl, _ = gelu_parts(u[:, PAIR:])
            mbuf[g, c, q] = (u[:, :PAIR] * gl).astype(BF16)
            m_y[c].start()
            m_p[c].start()

        def s4(c):
            m_y[c].wait_recv()
            m_f[c].start()

        def s5(c):
            if g == 0:
                need_weight(n_ch + c)
                w_copies[n_ch + c].wait()
            m_p[c].wait_recv()
            m_f[c].wait_recv()
            blocks = [mbuf[g, c, j] for j in range(4)]
            for j in range(4):
                m_ref[4 * c + j, rows, :] = blocks[j]
            m = jnp.concatenate(blocks, axis=1)
            for n in range(0, hid, 256):
                o = jnp.dot(m, w2b[c, :, n:n + 256], preferred_element_type=F32)
                if c:
                    facc[g, :, n:n + 256] += o
                else:
                    facc[g, :, n:n + 256] = o

        def u_gather():
            u_yy.start()
            u_p.start()

        def u_forward():
            u_yy.wait_recv()
            u_f.start()

        def u_done():
            u_p.wait_recv()
            u_f.wait_recv()

        def z1():
            for b in range(4):
                zsend[g, b] = facc[g, b * rz:(b + 1) * rz, :].astype(BF16)
            for d in (2, 1, 3):
                z_rs[d - 1].start()

        def z2():
            off = pl.multiple_of(z * rz, rz)
            f = facc[g, pl.ds(off, rz), :]
            for d in (1, 3, 2):
                z_rs[d - 1].wait_recv()
                f = f + zin[g, d - 1].astype(F32)
            f = f.astype(BF16)
            fsum[g, z] = f
            for d in (2, 1, 3):
                z_ag[d - 1].start()
            xoff = pl.multiple_of(row0 + z * rz, rz)
            r = ALPHA * x_ref[pl.ds(xoff, rz), :].astype(F32) + f.astype(F32) + b2_ref[...]
            gd = dy_ref[pl.ds(xoff, rz), :].astype(F32) * gam_ref[...]
            mean = jnp.sum(r, axis=1, keepdims=True) * (1.0 / hid)
            cen = r - mean
            m2 = jnp.sum(cen * cen, axis=1, keepdims=True)
            sg = jnp.sum(gd, axis=1, keepdims=True)
            sgr = jnp.sum(gd * cen, axis=1, keepdims=True)
            lane = lax.broadcasted_iota(jnp.int32, (rz, 128), 1)
            vals = jnp.where(lane == 0, mean, jnp.where(lane == 1, m2, jnp.where(lane == 2, sg, jnp.where(lane == 3, sgr, 0.0))))
            tmp[...] = jnp.zeros_like(tmp)
            tmp[pl.ds(off, rz), :] = vals
            stat_in[g, z, q] = tmp[...].T[:8, :]
            for s in st:
                s.start()

        def z3():
            for s in st:
                s.wait_recv()
            per = [sum(stat_in[g, a, h] for a in range(4)) for h in range(4)]
            mu = sum(p[0:1, :] for p in per) * 0.25
            m2 = sum(p[1:2, :] + float(hid) * (p[0:1, :] - mu) * (p[0:1, :] - mu) for p in per)
            rho = lax.rsqrt(m2 * (1.0 / hidden) + LN_EPS)
            mg = sum(p[2:3, :] for p in per) * (1.0 / hidden)
            mgr = rho * sum(p[3:4, :] + (p[0:1, :] - mu) * p[2:3, :] for p in per) * (1.0 / hidden)
            tmp[0:1, :] = mu
            tmp[1:2, :] = rho
            tmp[2:3, :] = mg
            tmp[3:4, :] = mgr
            cols = tmp[...].T
            tmp[...] = cols
            for d in range(3):
                z_ag[d].wait_recv()
            for b in range(4):
                rr = pl.ds(row0 + b * rz, rz)
                c4 = tmp[b * rz:(b + 1) * rz, :]
                r = ALPHA * x_ref[rr, :].astype(F32) + fsum[g, b].astype(F32) + b2_ref[...]
                dy = dy_ref[rr, :].astype(F32)
                rhat = (r - c4[:, 0:1]) * c4[:, 1:2]
                y_ref[rr, :] = (gam_ref[...] * rhat + bet_ref[...]).astype(BF16)
                dr = c4[:, 1:2] * (dy * gam_ref[...] - c4[:, 2:3] - rhat * c4[:, 3:4])
                dr_buf[rr, :] = dr
                d_ref[rr, :] = dr.astype(BF16)
                sums = (jnp.sum(dr, axis=0, keepdims=True), jnp.sum(dy * rhat, axis=0, keepdims=True), jnp.sum(dy, axis=0, keepdims=True))
                for out, s in zip((db2_ref, dgam_ref, dbet_ref), sums):
                    if g == 0 and b == 0:
                        out[...] = s
                    else:
                        out[...] += s

        def t1(c):
            for h in range(2):
                o = dot_nt(d_ref[rows, :], w2b[c, 256 * h:256 * (h + 1), :]).astype(BF16)
                npart[g, c, 0, h] = o[:, :PAIR]
                npart[g, c, 1, h] = o[:, PAIR:]
            n_d2d[c].start()

        def t2(c):
            n_d2d[c].wait_recv()
            nsend[g, c] = (npart[g, c, k, 1 - y].astype(F32) + nhalf[g, c, 1 - y].astype(F32)).astype(BF16)
            n_y[c].start()

        def t3(c):
            n_y[c].wait_recv()
            nbuf[g, c, q] = (npart[g, c, k, y].astype(F32) + nhalf[g, c, y].astype(F32) + nin[g, c].astype(F32)).astype(BF16)
            n_yy[c].start()
            n_p[c].start()

        def t4(c):
            n_yy[c].wait_recv()
            n_f[c].start()

        def t5(c):
            n_p[c].wait_recv()
            n_f[c].wait_recv()
            parts = []
            for j in range(4):
                dm = nbuf[g, c, j].astype(F32)
                u = ubuf[g, j, c].astype(F32)
                gl, slope = gelu_parts(u[:, PAIR:])
                dv = dm * gl
                dg = dm * u[:, :PAIR] * slope
                duf = jnp.concatenate([dv, dg], axis=1)
                s = jnp.sum(duf, axis=0, keepdims=True)
                if g == 0:
                    db1_ref[4 * c + j] = s
                else:
                    db1_ref[4 * c + j] += s
                du = duf.astype(BF16)
                du_ref[4 * c + j, rows, :] = du
                parts.append(du)
            du = jnp.concatenate(parts, axis=1)
            for n in range(0, hid, 256):
                o = dot_nt(du, w1b[c, n:n + 256, :])
                if c:
                    dxacc[rows, n:n + 256] += o
                else:
                    dxacc[rows, n:n + 256] = o

        fwd = [functools.partial(s1, 0)]
        for c in range(1, n_ch):
            fwd += [functools.partial(s1, c), functools.partial(s2, c - 1)]
        fwd += [functools.partial(s2, n_ch - 1), functools.partial(s3, 0)]
        for c in range(1, n_ch):
            fwd += [functools.partial(s3, c), functools.partial(s4, c - 1)]
            if c > 1:
                fwd += [functools.partial(s5, c - 2)]
        fwd += [u_gather, functools.partial(s5, n_ch - 2), functools.partial(s4, n_ch - 1), functools.partial(s5, n_ch - 1)]
        mid = [z1, z2, u_forward, z3]
        bwd = [functools.partial(t1, 0)]
        for c in range(1, n_ch):
            bwd += [functools.partial(t1, c), functools.partial(t2, c - 1)]
        bwd += [functools.partial(t2, n_ch - 1), u_done, functools.partial(t3, 0)]
        for c in range(1, n_ch):
            bwd += [functools.partial(t3, c), functools.partial(t4, c - 1)]
            if c > 1:
                bwd += [functools.partial(t5, c - 2)]
        bwd += [functools.partial(t5, n_ch - 2), functools.partial(t4, n_ch - 1), functools.partial(t5, n_ch - 1)]
        return fwd, mid, bwd

    groups = [make_group(g) for g in range(GROUPS)]
    for part in range(3):
        for fwd_mid_bwd in groups:
            for step in fwd_mid_bwd[part]:
                step()

    rt = tokens // 4
    for d, out in enumerate((dx0_ref, dx1_ref, dx2_ref, dx3_ref)):
        off = pl.multiple_of(lax.rem(z + d, 4) * rt, rt)
        o = dxacc[pl.ds(off, rt), :]
        if d == 0:
            drz_ref[...] = ALPHA * dr_buf[pl.ds(off, rt), :] + o
            out[...] = o.astype(BF16)
        else:
            out[...] = o.astype(BF16)
    for w in waits:
        w.wait_send()


def dw2_kernel(m_ref, d_ref, o_ref):
    for j in range(m_ref.shape[0]):
        o_ref[PAIR * j:PAIR * (j + 1), :] = dot_tn(m_ref[j], d_ref[...])


def dw1_kernel(x_ref, du_ref, y_in, db1_in, db2_in, dg_in, dbt_in, o_ref, y_ref, db1_ref, db2_ref, dg_ref, dbt_ref):
    for j in range(du_ref.shape[0]):
        o_ref[:, 2 * PAIR * j:2 * PAIR * (j + 1)] = dot_tn(x_ref[...], du_ref[j])

    @pl.when(pl.program_id(0) == 0)
    def _():
        y_ref[...] = y_in[...]
        db1_ref[...] = db1_in[...]
        db2_ref[...] = db2_in[...]
        dg_ref[...] = dg_in[...]
        dbt_ref[...] = dbt_in[...]


def place_kernel(a_ref, b_ref, c_ref, d_ref, o_ref):
    z = lax.axis_index('ff')
    rt = a_ref.shape[0]
    for d, ref in enumerate((a_ref, b_ref, c_ref, d_ref)):
        o_ref[pl.ds(pl.multiple_of(lax.rem(z + 4 - d, 4) * rt, rt), rt), :] = ref[...]


def solution(mesh):
    data_spec = P('dp', 'hd')
    hid_spec = P('hd')
    in_specs = (data_spec, P('hd', 'ff'), P('ff'), P('ff', 'hd'), hid_spec, hid_spec, hid_spec, data_spec)
    out_specs = (data_spec, data_spec, P(('dp', 'hd'), 'ff'), P(('dp', 'ff'), 'hd'), P(('dp', 'ff')), P(('dp', 'hd')), P(('dp', 'hd')), P(('dp', 'hd')))
    n_ff = mesh.shape['ff']
    vmem = pl.BlockSpec(memory_space=pltpu.VMEM)
    hbm = pl.BlockSpec(memory_space=pl.ANY)
    S = jax.ShapeDtypeStruct

    def device_step(x_loc, w_up, b_up, w_down, b_down, ln_gain, ln_bias, dy_loc):
        tokens, hid = x_loc.shape
        n_blocks = w_up.shape[1] // (2 * PAIR)
        n_ch = n_blocks // 4
        tn = tokens // GROUPS
        rt = tokens // 4
        g = GROUPS
        dma = pltpu.SemaphoreType.DMA
        outs = pl.pallas_call(
            main_kernel,
            out_shape=(
                S((tokens, hid), BF16), S((n_blocks, tokens, PAIR), BF16), S((tokens, hid), BF16), S((n_blocks, tokens, 2 * PAIR), BF16),
                S((rt, hid), BF16), S((rt, hid), BF16), S((rt, hid), BF16), S((rt, hid), BF16), S((rt, hid), F32),
                S((n_blocks, 1, 2 * PAIR), F32), S((1, hid), F32), S((1, hid), F32), S((1, hid), F32),
            ),
            in_specs=[vmem, hbm, vmem, hbm, vmem, vmem, vmem, vmem],
            out_specs=[vmem] * 13,
            scratch_shapes=[
                pltpu.VMEM((n_ch, hid, 8 * PAIR), BF16), pltpu.VMEM((n_ch, 4 * PAIR, hid), BF16),
                pltpu.VMEM((g, n_ch, 2, 2, tn, 2 * PAIR), BF16), pltpu.VMEM((g, n_ch, 2, tn, 2 * PAIR), BF16),
                pltpu.VMEM((g, n_ch, tn, 2 * PAIR), BF16), pltpu.VMEM((g, n_ch, tn, 2 * PAIR), BF16),
                pltpu.VMEM((g, 4, n_ch, tn, 2 * PAIR), BF16), pltpu.VMEM((g, n_ch, 4, tn, PAIR), BF16),
                pltpu.VMEM((g, tn, hid), F32), pltpu.VMEM((g, 4, tn // 4, hid), BF16), pltpu.VMEM((g, 3, tn // 4, hid), BF16),
                pltpu.VMEM((g, 4, tn // 4, hid), BF16), pltpu.VMEM((g, 4, 4, 8, 128), F32), pltpu.VMEM((128, 128), F32),
                pltpu.VMEM((tokens, hid), F32),
                pltpu.VMEM((g, n_ch, 2, 2, tn, PAIR), BF16), pltpu.VMEM((g, n_ch, 2, tn, PAIR), BF16),
                pltpu.VMEM((g, n_ch, tn, PAIR), BF16), pltpu.VMEM((g, n_ch, tn, PAIR), BF16),
                pltpu.VMEM((g, n_ch, 4, tn, PAIR), BF16), pltpu.VMEM((tokens, hid), F32),
                dma((2 * n_ch,)), dma((g, 10, n_ch)), dma((g, 10, n_ch)), dma((g, 3)), dma((g, 3)),
                dma((g, 2, 3)), dma((g, 2, 3)), dma((g, 15)), dma((g, 15)),
            ],
            compiler_params=pltpu.CompilerParams(collective_id=0, has_side_effects=True, vmem_limit_bytes=48 * 2**20),
            name='mlp_main',
        )(x_loc, w_up, b_up.reshape(n_blocks, 1, 2 * PAIR), w_down, b_down.reshape(1, hid), ln_gain.reshape(1, hid), ln_bias.reshape(1, hid), dy_loc)
        y_a, m_a, d_a, du_a, _, dx1, dx2, dx3, drz, db1, db2, dgam, dbet = outs

        def shift(v, d):
            return lax.ppermute(v, 'ff', [(i, (i + d) % n_ff) for i in range(n_ff)])

        parts = [shift(v, d + 1) for d, v in enumerate((dx1, dx2, dx3))]
        mb = 2
        dw_down = pl.pallas_call(
            dw2_kernel,
            grid=(n_blocks // mb,),
            out_shape=S((n_blocks * PAIR, hid), F32),
            in_specs=[pl.BlockSpec((mb, tokens, PAIR), lambda i: (i, 0, 0)), vmem],
            out_specs=pl.BlockSpec((mb * PAIR, hid), lambda i: (i, 0)),
            cost_estimate=pl.CostEstimate(flops=2 * tokens * n_blocks * PAIR * hid * 3, bytes_accessed=4 * n_blocks * PAIR * hid, transcendentals=0),
            name='mlp_dw2',
        )(m_a, d_a)
        own = (drz + sum(p.astype(F32) for p in parts)).astype(BF16)
        back = [shift(own, d) for d in (1, 2, 3)]
        hb = PAIR
        dw_up, y_o, db1_o, db2_o, dg_o, dbt_o = pl.pallas_call(
            dw1_kernel,
            grid=(hid // hb,),
            out_shape=(S((hid, n_blocks * 2 * PAIR), F32), S(y_a.shape, BF16), S(db1.shape, F32), S(db2.shape, F32), S(db2.shape, F32), S(db2.shape, F32)),
            in_specs=[pl.BlockSpec((tokens, hb), lambda i: (0, i)), vmem, vmem, vmem, vmem, vmem, vmem],
            out_specs=[pl.BlockSpec((hb, n_blocks * 2 * PAIR), lambda i: (i, 0)), vmem, vmem, vmem, vmem, vmem],
            cost_estimate=pl.CostEstimate(flops=2 * tokens * n_blocks * 2 * PAIR * hid * 3, bytes_accessed=8 * n_blocks * PAIR * hid, transcendentals=0),
            name='mlp_dw1',
        )(x_loc, du_a, y_a, db1, db2, dgam, dbet)
        dx = pl.pallas_call(
            place_kernel,
            out_shape=S((tokens, hid), BF16),
            in_specs=[vmem] * 4,
            out_specs=vmem,
            name='mlp_place',
        )(own, *back)
        return (y_o, dx, dw_up, dw_down, db1_o.reshape(-1), db2_o.reshape(-1), dg_o.reshape(-1), dbt_o.reshape(-1))

    return jax.shard_map(device_step, mesh=mesh, in_specs=in_specs, out_specs=out_specs, check_vma=False)
```

```python
import functools
import math

import jax
import jax.numpy as jnp
from jax import lax
from jax.experimental import pallas as pl
from jax.experimental.pallas import tpu as pltpu
from jax.sharding import PartitionSpec as P

PAIR = 128
ALPHA = math.sqrt(140.0)
LN_EPS = 1e-5
GELU_K = math.sqrt(2.0 / math.pi)
GELU_C = 0.044715
MESH = pl.DeviceIdType.MESH
F32 = jnp.float32
BF16 = jnp.bfloat16

GROUPS = 1
VMEM_LIMIT = 60 * 2**20
LOOKAHEAD = 3


def gelu_parts(z):
    t = jnp.tanh(GELU_K * (z + GELU_C * (z * z * z)))
    cdf = 0.5 * (1.0 + t)
    slope = cdf + z * (0.5 * (1.0 - t * t) * (GELU_K * (1.0 + (3.0 * GELU_C) * (z * z))))
    return z * cdf, slope


def dot_nt(a, b):
    return lax.dot_general(a, b, (((1,), (1,)), ((), ())), preferred_element_type=F32)


def dot_tn(a, b):
    return lax.dot_general(a, b, (((0,), (0,)), ((), ())), preferred_element_type=F32)


def main_kernel(
    x_hbm, w1_hbm, b1_hbm, w2_hbm, b2_hbm, gam_hbm, bet_hbm, dy_hbm,
    y_hbm, m_hbm, d_hbm, du_hbm, xg_hbm, db1_hbm, dsm_hbm,
    y_ref, m_ref, d_ref, du_ref, db1_ref, dsm_ref,
    x_ref, dy_ref, b1_ref, b2_ref, gam_ref, bet_ref,
    w1b, w2b, upart, uhalf, usend, uin, ubuf, mbuf, facc, zsend, zin, fsum, stat_in, stat_all, tmp, dr_buf,
    npart, nhalf, nsend, nin, nbuf, dxacc, xsend, xin, xown,
    wsem, isem, osem, chunk_s, chunk_r, full_s, full_r, zsem_s, zsem_r,
):
    n_ch = w1b.shape[0]
    tokens, hid = x_ref.shape
    hidden = 4 * hid
    tn = tokens // GROUPS
    rz = tn // 4
    cw = 8 * PAIR
    q = lax.axis_index('hd')
    z = lax.axis_index('ff')
    k = lax.rem(q, 2)
    y = lax.div(q, 2)
    pq = q + 1 - 2 * k
    yq = lax.rem(q + 2, 4)

    def remote(src, dst, ss, rs, **dev):
        return pltpu.make_async_remote_copy(src_ref=src, dst_ref=dst, send_sem=ss, recv_sem=rs, device_id=dev, device_id_type=MESH)

    w_copies = [pltpu.make_async_copy(w1_hbm.at[:, pl.ds(cw * c, cw)], w1b.at[c], wsem.at[c]) for c in range(n_ch)]
    w_copies += [pltpu.make_async_copy(w2_hbm.at[pl.ds(4 * PAIR * c, 4 * PAIR), :], w2b.at[c], wsem.at[n_ch + c]) for c in range(n_ch)]
    in_copies = [pltpu.make_async_copy(a, b, isem.at[i]) for i, (a, b) in enumerate(((x_hbm, x_ref), (b1_hbm, b1_ref), (dy_hbm, dy_ref), (b2_hbm, b2_ref), (gam_hbm, gam_ref), (bet_hbm, bet_ref)))]
    started = [0]
    landed = set()

    def need_weight(i):
        while started[0] < min(i + LOOKAHEAD, 2 * n_ch):
            w_copies[started[0]].start()
            started[0] += 1
        if i not in landed:
            landed.add(i)
            w_copies[i].wait()

    bar = pltpu.get_barrier_semaphore()
    for d in range(1, 4):
        pl.semaphore_signal(bar, inc=1, device_id={'ff': lax.rem(z + d, 4)}, device_id_type=MESH)
    for d in range(1, 4):
        pl.semaphore_signal(bar, inc=1, device_id={'hd': lax.rem(q + d, 4)}, device_id_type=MESH)
    in_copies[0].start()
    for i in range(LOOKAHEAD):
        w_copies[i].start()
    started[0] = LOOKAHEAD
    for cp in in_copies[1:]:
        cp.start()

    tmp[...] = jnp.zeros_like(tmp)
    waits = []
    outs = []

    def put(src, dst):
        cp = pltpu.make_async_copy(src, dst, osem.at[len(outs)])
        cp.start()
        outs.append(cp)

    seen = set()

    def once(name):
        new = name not in seen
        seen.add(name)
        return new

    def make_group(g):
        row0 = g * tn
        rows = pl.ds(row0, tn)

        def ch(kind, c):
            return chunk_s.at[g, kind, c], chunk_r.at[g, kind, c]

        u_d2d = [remote(upart.at[g, c, 1 - k], uhalf.at[g, c], *ch(0, c), hd=pq) for c in range(n_ch)]
        u_y = [remote(usend.at[g, c], uin.at[g, c], *ch(1, c), hd=yq) for c in range(n_ch)]
        m_p = [remote(mbuf.at[g, c, q], mbuf.at[g, c, q], *ch(2, c), hd=pq) for c in range(n_ch)]
        m_y = [remote(mbuf.at[g, c, q], mbuf.at[g, c, q], *ch(3, c), hd=yq) for c in range(n_ch)]
        m_f = [remote(mbuf.at[g, c, yq], mbuf.at[g, c, yq], *ch(4, c), hd=pq) for c in range(n_ch)]
        n_d2d = [remote(npart.at[g, c, 1 - k], nhalf.at[g, c], *ch(5, c), hd=pq) for c in range(n_ch)]
        n_y = [remote(nsend.at[g, c], nin.at[g, c], *ch(6, c), hd=yq) for c in range(n_ch)]
        n_p = [remote(nbuf.at[g, c, q], nbuf.at[g, c, q], *ch(7, c), hd=pq) for c in range(n_ch)]
        n_yy = [remote(nbuf.at[g, c, q], nbuf.at[g, c, q], *ch(8, c), hd=yq) for c in range(n_ch)]
        n_f = [remote(nbuf.at[g, c, yq], nbuf.at[g, c, yq], *ch(9, c), hd=pq) for c in range(n_ch)]
        u_p = remote(ubuf.at[g, q], ubuf.at[g, q], full_s.at[g, 0], full_r.at[g, 0], hd=pq)
        u_yy = remote(ubuf.at[g, q], ubuf.at[g, q], full_s.at[g, 1], full_r.at[g, 1], hd=yq)
        u_f = remote(ubuf.at[g, yq], ubuf.at[g, yq], full_s.at[g, 2], full_r.at[g, 2], hd=pq)

        def zc(kind, src, dst):
            return [remote(src(d), dst(d), zsem_s.at[g, kind, d - 1], zsem_r.at[g, kind, d - 1], ff=lax.rem(z + d, 4)) for d in range(1, 4)]

        z_rs = zc(0, lambda d: zsend.at[g, lax.rem(z + d, 4)], lambda d: zin.at[g, d - 1])
        z_ag = zc(1, lambda d: fsum.at[g, z], lambda d: fsum.at[g, z])
        z_st = zc(2, lambda d: stat_all.at[g, z], lambda d: stat_all.at[g, z])
        x_rs = zc(3, lambda d: xsend.at[g, lax.rem(z + d, 4)], lambda d: xin.at[g, d - 1])
        st = [remote(stat_in.at[g, q], stat_in.at[g, q], zsem_s.at[g, 5, d - 1], zsem_r.at[g, 5, d - 1], hd=lax.rem(q + d, 4)) for d in range(1, 4)]
        waits.extend(u_d2d + u_y + m_p + m_y + m_f + n_d2d + n_y + n_p + n_yy + n_f + [u_p, u_yy, u_f] + z_rs + z_ag + z_st + x_rs + st)

        def s1(c):
            if once('x'):
                in_copies[0].wait()
            need_weight(c)
            for j in range(4):
                o = jnp.dot(x_ref[rows, :], w1b[c, :, 2 * PAIR * j:2 * PAIR * (j + 1)], preferred_element_type=F32)
                upart[g, c, j % 2, j // 2] = o.astype(BF16)

        def sd(c):
            u_d2d[c].start()

        def s2(c):
            u_d2d[c].wait_recv()
            usend[g, c] = (upart[g, c, k, 1 - y].astype(F32) + uhalf[g, c, 1 - y].astype(F32)).astype(BF16)
            u_y[c].start()

        def s3(c):
            if once('in'):
                for cp in in_copies[1:]:
                    cp.wait()
            u_y[c].wait_recv()
            u = upart[g, c, k, y].astype(F32) + uhalf[g, c, y].astype(F32) + uin[g, c].astype(F32)
            u = (u + b1_ref[4 * c + q]).astype(BF16)
            ubuf[g, q, c] = u
            u = u.astype(F32)
            gl, _ = gelu_parts(u[:, PAIR:])
            mbuf[g, c, q] = (u[:, :PAIR] * gl).astype(BF16)
            m_y[c].start()
            m_p[c].start()

        def s4(c):
            m_y[c].wait_recv()
            m_f[c].start()

        def s5(c):
            need_weight(n_ch + c)
            m_p[c].wait_recv()
            m_f[c].wait_recv()
            blocks = [mbuf[g, c, j] for j in range(4)]
            for j in range(4):
                m_ref[4 * c + j, rows, :] = blocks[j]
            m = jnp.concatenate(blocks, axis=1)
            for n in range(0, hid, 256):
                o = jnp.dot(m, w2b[c, :, n:n + 256], preferred_element_type=F32)
                if c:
                    facc[g, :, n:n + 256] += o
                else:
                    facc[g, :, n:n + 256] = o

        def ug():
            u_yy.start()
            u_p.start()

        def uf():
            u_yy.wait_recv()
            u_f.start()

        def ud():
            u_p.wait_recv()
            u_f.wait_recv()

        def z1():
            for b in range(4):
                zsend[g, b] = facc[g, b * rz:(b + 1) * rz, :].astype(BF16)
            for d in (2, 1, 3):
                z_rs[d - 1].start()

        def z2():
            off = pl.multiple_of(z * rz, rz)
            f = facc[g, pl.ds(off, rz), :]
            for d in (1, 3, 2):
                z_rs[d - 1].wait_recv()
                f = f + zin[g, d - 1].astype(F32)
            f = f.astype(BF16)
            fsum[g, z] = f
            for d in (2, 1, 3):
                z_ag[d - 1].start()
            xoff = pl.multiple_of(row0 + z * rz, rz)
            r = ALPHA * x_ref[pl.ds(xoff, rz), :].astype(F32) + f.astype(F32) + b2_ref[...]
            gd = dy_ref[pl.ds(xoff, rz), :].astype(F32) * gam_ref[...]
            mean = jnp.sum(r, axis=1, keepdims=True) * (1.0 / hid)
            cen = r - mean
            m2 = jnp.sum(cen * cen, axis=1, keepdims=True)
            sg = jnp.sum(gd, axis=1, keepdims=True)
            sgr = jnp.sum(gd * cen, axis=1, keepdims=True)
            lane = lax.broadcasted_iota(jnp.int32, (rz, 128), 1)
            vals = jnp.where(lane == 0, mean, jnp.where(lane == 1, m2, jnp.where(lane == 2, sg, jnp.where(lane == 3, sgr, 0.0))))
            stat_in[g, q] = vals
            for s in st:
                s.start()

        def zb():
            for s in st:
                s.wait_recv()
            per = [stat_in[g, h] for h in range(4)]
            mu = sum(p[:, 0:1] for p in per) * 0.25
            m2 = sum(p[:, 1:2] + float(hid) * (p[:, 0:1] - mu) * (p[:, 0:1] - mu) for p in per)
            rho = lax.rsqrt(m2 * (1.0 / hidden) + LN_EPS)
            mg = sum(p[:, 2:3] for p in per) * (1.0 / hidden)
            mgr = rho * sum(p[:, 3:4] + (p[:, 0:1] - mu) * p[:, 2:3] for p in per) * (1.0 / hidden)
            lane = lax.broadcasted_iota(jnp.int32, (rz, 128), 1)
            tmp[:rz, :] = jnp.where(lane == 0, mu, jnp.where(lane == 1, rho, jnp.where(lane == 2, mg, jnp.where(lane == 3, mgr, 0.0))))
            stat_all[g, z] = tmp[...].T[:8, :]
            for s in z_st:
                s.start()

        def z3():
            for s in z_ag + z_st:
                s.wait_recv()
            for b in range(4):
                tmp[8 * b:8 * (b + 1), :] = stat_all[g, b]
            cols = tmp[...].T
            for b in range(4):
                rr = pl.ds(row0 + b * rz, rz)
                c4 = cols[:rz, 8 * b:8 * b + 4]
                r = ALPHA * x_ref[rr, :].astype(F32) + fsum[g, b].astype(F32) + b2_ref[...]
                dy = dy_ref[rr, :].astype(F32)
                rhat = (r - c4[:, 0:1]) * c4[:, 1:2]
                y_ref[rr, :] = (gam_ref[...] * rhat + bet_ref[...]).astype(BF16)
                dr = c4[:, 1:2] * (dy * gam_ref[...] - c4[:, 2:3] - rhat * c4[:, 3:4])
                dr_buf[rr, :] = dr
                d_ref[rr, :] = dr.astype(BF16)
                sums = (jnp.sum(dr, axis=0, keepdims=True), jnp.sum(dy * rhat, axis=0, keepdims=True), jnp.sum(dy, axis=0, keepdims=True))
                for i, s in enumerate(sums):
                    if g == 0 and b == 0:
                        dsm_ref[i] = s
                    else:
                        dsm_ref[i] += s

        def t1(c):
            for h in range(2):
                o = dot_nt(d_ref[rows, :], w2b[c, 256 * h:256 * (h + 1), :]).astype(BF16)
                npart[g, c, 0, h] = o[:, :PAIR]
                npart[g, c, 1, h] = o[:, PAIR:]
            n_d2d[c].start()
            if c == n_ch - 1:
                put(y_ref.at[rows, :], y_hbm.at[rows, :])
                put(d_ref.at[rows, :], d_hbm.at[rows, :])

        def t2(c):
            n_d2d[c].wait_recv()
            nsend[g, c] = (npart[g, c, k, 1 - y].astype(F32) + nhalf[g, c, 1 - y].astype(F32)).astype(BF16)
            n_y[c].start()

        def t3(c):
            n_y[c].wait_recv()
            nbuf[g, c, q] = (npart[g, c, k, y].astype(F32) + nhalf[g, c, y].astype(F32) + nin[g, c].astype(F32)).astype(BF16)
            n_yy[c].start()
            n_p[c].start()

        def t4(c):
            n_yy[c].wait_recv()
            n_f[c].start()

        def t5(c):
            n_p[c].wait_recv()
            n_f[c].wait_recv()
            parts = []
            for j in range(4):
                dm = nbuf[g, c, j].astype(F32)
                u = ubuf[g, j, c].astype(F32)
                gl, slope = gelu_parts(u[:, PAIR:])
                dv = dm * gl
                dg = dm * u[:, :PAIR] * slope
                duf = jnp.concatenate([dv, dg], axis=1)
                s = jnp.sum(duf, axis=0, keepdims=True)
                if g == 0:
                    db1_ref[4 * c + j] = s
                else:
                    db1_ref[4 * c + j] += s
                du = duf.astype(BF16)
                du_ref[4 * c + j, rows, :] = du
                parts.append(du)
            du = jnp.concatenate(parts, axis=1)
            for n in range(0, hid, 256):
                o = dot_nt(du, w1b[c, n:n + 256, :])
                if c:
                    dxacc[rows, n:n + 256] += o
                else:
                    dxacc[rows, n:n + 256] = o
            put(du_ref.at[pl.ds(4 * c, 4), rows, :], du_hbm.at[pl.ds(4 * c, 4), rows, :])

        def x1():
            put(db1_ref, db1_hbm)
            put(dsm_ref, dsm_hbm)
            for b in range(4):
                xsend[g, b] = dxacc[row0 + b * rz:row0 + (b + 1) * rz, :].astype(BF16)
            for d in (2, 1, 3):
                x_rs[d - 1].start()

        def x2():
            off = pl.multiple_of(row0 + z * rz, rz)
            t = ALPHA * dr_buf[pl.ds(off, rz), :] + dxacc[pl.ds(off, rz), :]
            for d in (1, 3, 2):
                x_rs[d - 1].wait_recv()
                t = t + xin[g, d - 1].astype(F32)
            t = t.astype(BF16)
            xown[g] = t
            for b in range(4):
                put(xown.at[g], xg_hbm.at[b])

        return dict(s1=s1, sd=sd, s2=s2, s3=s3, s4=s4, s5=s5, ug=ug, uf=uf, ud=ud, z1=z1, z2=z2, zb=zb, z3=z3, t1=t1, t2=t2, t3=t3, t4=t4, t5=t5, x1=x1, x2=x2)

    groups = {n: make_group(i) for i, n in enumerate('AB'[:GROUPS])}
    for name in order(n_ch):
        with jax.named_scope(name):
            if name == 'barrier':
                pl.semaphore_wait(bar, 6)
            elif name == 'mout':
                put(m_ref, m_hbm)
            else:
                groups[name[2]][name[:2]](*map(int, name[3:]))
    with jax.named_scope('finish'):
        for w in waits:
            w.wait_send()
        for w in outs:
            w.wait()


def order(n):
    def seq(name):
        return [f'{name}A{c}' for c in range(n)]

    o = ['s1A0', 'barrier', 'sdA0']
    for c in range(1, n):
        o += [f's1A{c}', f'sdA{c}', f's2A{c - 1}']
    o += [f's2A{n - 1}'] + seq('s3') + ['s4A0', 's4A1']
    for c in range(n):
        o += [f's5A{c}'] + ([f's4A{c + 2}'] if c + 2 < n else [])
    o += ['z1A', 'ugA', 'mout', 'z2A', 'zbA', 'ufA', 'z3A', 't1A0']
    for c in range(1, n):
        o += [f't1A{c}', f't2A{c - 1}']
    o += [f't2A{n - 1}', 'udA'] + seq('t3') + ['t4A0', 't4A1']
    for c in range(n):
        o += [f't5A{c}'] + ([f't4A{c + 2}'] if c + 2 < n else [])
    return o + ['x1A', 'x2A']


def grad_kernel(
    m_hbm, d_hbm, x_hbm, du_hbm, y_in, db1_in, dsm_in,
    dw1_hbm, dw2_hbm, y_hbm, db1_hbm, db2_hbm, dgam_hbm, dbet_hbm,
    m_ref, d_ref, x_ref, du_ref, y_ref, db1_ref, dsm_ref, dw1b, dw2b, isem, sem,
):
    n_blocks = m_ref.shape[0]
    hid = x_ref.shape[1]
    n_ch = n_blocks // 4
    copies = []
    loads = []

    def get(src, dst):
        cp = pltpu.make_async_copy(src, dst, isem.at[len(loads)])
        cp.start()
        loads.append(cp)

    def put(src, dst):
        cp = pltpu.make_async_copy(src, dst, sem.at[len(copies)])
        cp.start()
        copies.append(cp)

    get(d_hbm, d_ref)
    for c in range(n_ch):
        get(m_hbm.at[pl.ds(4 * c, 4)], m_ref.at[pl.ds(4 * c, 4)])
    loads[0].wait()
    for c in range(n_ch):
        loads[1 + c].wait()
        for i in range(4 * c, 4 * c + 4, 2):
            for j in range(2):
                dw2b[PAIR * (i + j):PAIR * (i + j + 1), :] = dot_tn(m_ref[i + j], d_ref[...])
            put(dw2b.at[pl.ds(PAIR * i, 2 * PAIR), :], dw2_hbm.at[pl.ds(PAIR * i, 2 * PAIR), :])
        if c == 0:
            for a, b in ((x_hbm, x_ref), (du_hbm, du_ref), (y_in, y_ref), (db1_in, db1_ref), (dsm_in, dsm_ref)):
                get(a, b)
    loads[1 + n_ch].wait()
    loads[2 + n_ch].wait()
    for i in range(0, hid, PAIR):
        for j in range(n_blocks):
            dw1b[i:i + PAIR, 2 * PAIR * j:2 * PAIR * (j + 1)] = dot_tn(x_ref[:, i:i + PAIR], du_ref[j])
        put(dw1b.at[pl.ds(i, PAIR), :], dw1_hbm.at[pl.ds(i, PAIR), :])
    for cp in loads[3 + n_ch:]:
        cp.wait()
    for a, b in ((y_ref, y_hbm), (db1_ref, db1_hbm), (dsm_ref.at[0], db2_hbm), (dsm_ref.at[1], dgam_hbm), (dsm_ref.at[2], dbet_hbm)):
        put(a, b)
    for cp in copies:
        cp.wait()


def solution(mesh):
    data_spec = P('dp', 'hd')
    hid_spec = P('hd')
    in_specs = (data_spec, P('hd', 'ff'), P('ff'), P('ff', 'hd'), hid_spec, hid_spec, hid_spec, data_spec)
    out_specs = (data_spec, data_spec, P(('dp', 'hd'), 'ff'), P(('dp', 'ff'), 'hd'), P(('dp', 'ff')), P(('dp', 'hd')), P(('dp', 'hd')), P(('dp', 'hd')))
    hbm = pl.BlockSpec(memory_space=pltpu.HBM)
    S = jax.ShapeDtypeStruct

    def device_step(x_loc, w_up, b_up, w_down, b_down, ln_gain, ln_bias, dy_loc):
        tokens, hid = x_loc.shape
        n_blocks = w_up.shape[1] // (2 * PAIR)
        n_ch = n_blocks // 4
        tn = tokens // GROUPS
        g = GROUPS
        rz = tn // 4
        V = pltpu.VMEM
        dma = pltpu.SemaphoreType.DMA
        outs = pl.pallas_call(
            main_kernel,
            out_shape=(
                S((tokens, hid), BF16), S((n_blocks, tokens, PAIR), BF16), S((tokens, hid), BF16), S((n_blocks, tokens, 2 * PAIR), BF16),
                S((4, rz, hid), BF16), S((n_blocks, 1, 2 * PAIR), F32), S((3, 1, hid), F32),
            ),
            in_specs=[hbm] * 8,
            out_specs=[hbm] * 7,
            scratch_shapes=[
                V((tokens, hid), BF16), V((n_blocks, tokens, PAIR), BF16), V((tokens, hid), BF16), V((n_blocks, tokens, 2 * PAIR), BF16),
                V((n_blocks, 1, 2 * PAIR), F32), V((3, 1, hid), F32),
                V((tokens, hid), BF16), V((tokens, hid), BF16), V((n_blocks, 1, 2 * PAIR), F32), V((1, hid), F32), V((1, hid), F32), V((1, hid), F32),
                V((n_ch, hid, 8 * PAIR), BF16), V((n_ch, 4 * PAIR, hid), BF16),
                V((g, n_ch, 2, 2, tn, 2 * PAIR), BF16), V((g, n_ch, 2, tn, 2 * PAIR), BF16), V((g, n_ch, tn, 2 * PAIR), BF16), V((g, n_ch, tn, 2 * PAIR), BF16),
                V((g, 4, n_ch, tn, 2 * PAIR), BF16), V((g, n_ch, 4, tn, PAIR), BF16),
                V((g, tn, hid), F32), V((g, 4, rz, hid), BF16), V((g, 3, rz, hid), BF16), V((g, 4, rz, hid), BF16),
                V((g, 4, rz, 128), F32), V((g, 4, 8, 128), F32), V((128, 128), F32), V((tokens, hid), F32),
                V((g, n_ch, 2, 2, tn, PAIR), BF16), V((g, n_ch, 2, tn, PAIR), BF16), V((g, n_ch, tn, PAIR), BF16), V((g, n_ch, tn, PAIR), BF16),
                V((g, n_ch, 4, tn, PAIR), BF16), V((tokens, hid), F32),
                V((g, 4, rz, hid), BF16), V((g, 3, rz, hid), BF16), V((g, rz, hid), BF16),
                dma((2 * n_ch,)), dma((6,)), dma(((2 + n_ch) * g + 7,)), dma((g, 10, n_ch)), dma((g, 10, n_ch)), dma((g, 3)), dma((g, 3)), dma((g, 6, 3)), dma((g, 6, 3)),
            ],
            compiler_params=pltpu.CompilerParams(collective_id=0, has_side_effects=True, vmem_limit_bytes=VMEM_LIMIT),
            name='mlp_main',
        )(x_loc, w_up, b_up.reshape(n_blocks, 1, 2 * PAIR), w_down, b_down.reshape(1, hid), ln_gain.reshape(1, hid), ln_bias.reshape(1, hid), dy_loc)
        y_a, m_a, d_a, du_a, xg, db1, dsm = outs
        dx = lax.all_to_all(xg, 'ff', 0, 0)
        vec = S((1, hid), F32)
        dw_up, dw_down, y_o, db1_o, db2_o, dg_o, dbt_o = pl.pallas_call(
            grad_kernel,
            out_shape=(S((hid, n_blocks * 2 * PAIR), F32), S((n_blocks * PAIR, hid), F32), S(y_a.shape, BF16), S(db1.shape, F32), vec, vec, vec),
            in_specs=[hbm] * 7,
            out_specs=[hbm] * 7,
            scratch_shapes=[
                V((n_blocks, tokens, PAIR), BF16), V((tokens, hid), BF16), V((tokens, hid), BF16), V((n_blocks, tokens, 2 * PAIR), BF16),
                V((tokens, hid), BF16), V((n_blocks, 1, 2 * PAIR), F32), V((3, 1, hid), F32),
                V((hid, n_blocks * 2 * PAIR), F32), V((n_blocks * PAIR, hid), F32), dma((6 + n_ch,)), dma((n_blocks // 2 + hid // PAIR + 5,)),
            ],
            compiler_params=pltpu.CompilerParams(vmem_limit_bytes=VMEM_LIMIT),
            cost_estimate=pl.CostEstimate(flops=10**10, bytes_accessed=10**7, transcendentals=0),
            name='mlp_grads',
        )(m_a, d_a, x_loc, du_a, y_a, db1, dsm)
        return (y_o, dx.reshape(tokens, hid), dw_up, dw_down, db1_o.reshape(-1), db2_o.reshape(-1), dg_o.reshape(-1), dbt_o.reshape(-1))

    return jax.shard_map(device_step, mesh=mesh, in_specs=in_specs, out_specs=out_specs, check_vma=False)
```

```python
import functools
import math

import jax
import jax.numpy as jnp
from jax import lax
from jax.experimental import pallas as pl
from jax.experimental.pallas import tpu as pltpu
from jax.sharding import PartitionSpec as P

PAIR = 128
ALPHA = math.sqrt(140.0)
LN_EPS = 1e-5
GELU_K = math.sqrt(2.0 / math.pi)
GELU_C = 0.044715
MESH = pl.DeviceIdType.MESH
F32 = jnp.float32
BF16 = jnp.bfloat16

GROUPS = 1
VMEM_LIMIT = 60 * 2**20
LOOKAHEAD = 3


def gelu_parts(z):
    t = jnp.tanh(GELU_K * (z + GELU_C * (z * z * z)))
    cdf = 0.5 * (1.0 + t)
    slope = cdf + z * (0.5 * (1.0 - t * t) * (GELU_K * (1.0 + (3.0 * GELU_C) * (z * z))))
    return z * cdf, slope


def dot_nt(a, b):
    return lax.dot_general(a, b, (((1,), (1,)), ((), ())), preferred_element_type=F32)


def dot_tn(a, b):
    return lax.dot_general(a, b, (((0,), (0,)), ((), ())), preferred_element_type=F32)


def main_kernel(
    x_hbm, w1_hbm, b1_hbm, w2_hbm, b2_hbm, gam_hbm, bet_hbm, dy_hbm,
    y_hbm, m_hbm, d_hbm, du_hbm, xg_hbm, db1_hbm, dsm_hbm,
    y_ref, m_ref, d_ref, du_ref, db1_ref, dsm_ref,
    x_ref, dy_ref, b1_ref, b2_ref, gam_ref, bet_ref,
    w1b, w2b, upart, uhalf, usend, uin, ubuf, mbuf, facc, zsend, zin, fsum, stat_in, stat_all, tmp, dr_buf,
    npart, nhalf, nsend, nin, nbuf, dxacc, xsend, xin, xown,
    wsem, isem, osem, chunk_s, chunk_r, full_s, full_r, zsem_s, zsem_r,
):
    n_ch = w1b.shape[0]
    tokens, hid = x_ref.shape
    hidden = 4 * hid
    tn = tokens // GROUPS
    rz = tn // 4
    cw = 8 * PAIR
    q = lax.axis_index('hd')
    z = lax.axis_index('ff')
    k = lax.rem(q, 2)
    y = lax.div(q, 2)
    pq = q + 1 - 2 * k
    yq = lax.rem(q + 2, 4)
    dq = lax.rem(pq + 2, 4)
    last = n_ch - 1

    def remote(src, dst, ss, rs, **dev):
        return pltpu.make_async_remote_copy(src_ref=src, dst_ref=dst, send_sem=ss, recv_sem=rs, device_id=dev, device_id_type=MESH)

    w_copies = [pltpu.make_async_copy(w1_hbm.at[:, pl.ds(cw * c, cw)], w1b.at[c], wsem.at[c]) for c in range(n_ch)]
    w_copies += [pltpu.make_async_copy(w2_hbm.at[pl.ds(4 * PAIR * c, 4 * PAIR), :], w2b.at[c], wsem.at[n_ch + c]) for c in range(n_ch)]
    in_copies = [pltpu.make_async_copy(a, b, isem.at[i]) for i, (a, b) in enumerate(((x_hbm, x_ref), (b1_hbm, b1_ref), (dy_hbm, dy_ref), (b2_hbm, b2_ref), (gam_hbm, gam_ref), (bet_hbm, bet_ref)))]
    started = [0]
    landed = set()

    def need_weight(i):
        while started[0] < min(i + LOOKAHEAD, 2 * n_ch):
            w_copies[started[0]].start()
            started[0] += 1
        if i not in landed:
            landed.add(i)
            w_copies[i].wait()

    bar = pltpu.get_barrier_semaphore()
    for d in range(1, 4):
        pl.semaphore_signal(bar, inc=1, device_id={'ff': lax.rem(z + d, 4)}, device_id_type=MESH)
    for d in range(1, 4):
        pl.semaphore_signal(bar, inc=1, device_id={'hd': lax.rem(q + d, 4)}, device_id_type=MESH)
    in_copies[0].start()
    for i in range(LOOKAHEAD):
        w_copies[i].start()
    started[0] = LOOKAHEAD
    for cp in in_copies[1:]:
        cp.start()

    tmp[...] = jnp.zeros_like(tmp)
    waits = []
    outs = []

    def put(src, dst):
        cp = pltpu.make_async_copy(src, dst, osem.at[len(outs)])
        cp.start()
        outs.append(cp)

    seen = set()

    def once(name):
        new = name not in seen
        seen.add(name)
        return new

    def make_group(g):
        row0 = g * tn
        rows = pl.ds(row0, tn)

        def ch(kind, c):
            return chunk_s.at[g, kind, c], chunk_r.at[g, kind, c]

        u_d2d = [remote(upart.at[g, c, 1 - k], uhalf.at[g, c], *ch(0, c), hd=pq) for c in range(n_ch)]
        u_y = [remote(usend.at[g, c], uin.at[g, c], *ch(1, c), hd=yq) for c in range(n_ch)]
        m_p = [remote(mbuf.at[g, c, q], mbuf.at[g, c, q], *ch(2, c), hd=pq) for c in range(n_ch)]
        m_y = [remote(mbuf.at[g, c, q], mbuf.at[g, c, q], *ch(3, c), hd=yq) for c in range(n_ch)]
        m_f = [remote(mbuf.at[g, c, yq], mbuf.at[g, c, yq], *ch(4, c), hd=pq) for c in range(last)]
        m_f.append(remote(mbuf.at[g, last, q], mbuf.at[g, last, q], *ch(4, last), hd=dq))
        n_d2d = [remote(npart.at[g, c, 1 - k], nhalf.at[g, c], *ch(5, c), hd=pq) for c in range(n_ch)]
        n_y = [remote(nsend.at[g, c], nin.at[g, c], *ch(6, c), hd=yq) for c in range(n_ch)]
        n_p = [remote(nbuf.at[g, c, q], nbuf.at[g, c, q], *ch(7, c), hd=pq) for c in range(n_ch)]
        n_yy = [remote(nbuf.at[g, c, q], nbuf.at[g, c, q], *ch(8, c), hd=yq) for c in range(n_ch)]
        n_f = [remote(nbuf.at[g, c, yq], nbuf.at[g, c, yq], *ch(9, c), hd=pq) for c in range(last)]
        n_f.append(remote(nbuf.at[g, last, q], nbuf.at[g, last, q], *ch(9, last), hd=dq))
        u_p = remote(ubuf.at[g, q], ubuf.at[g, q], full_s.at[g, 0], full_r.at[g, 0], hd=pq)
        u_yy = remote(ubuf.at[g, q], ubuf.at[g, q], full_s.at[g, 1], full_r.at[g, 1], hd=yq)
        u_f = remote(ubuf.at[g, yq], ubuf.at[g, yq], full_s.at[g, 2], full_r.at[g, 2], hd=pq)

        def zc(kind, src, dst):
            return [remote(src(d), dst(d), zsem_s.at[g, kind, d - 1], zsem_r.at[g, kind, d - 1], ff=lax.rem(z + d, 4)) for d in range(1, 4)]

        z_rs = zc(0, lambda d: zsend.at[g, lax.rem(z + d, 4)], lambda d: zin.at[g, d - 1])
        z_ag = zc(1, lambda d: fsum.at[g, z], lambda d: fsum.at[g, z])
        z_st = zc(2, lambda d: stat_all.at[g, z], lambda d: stat_all.at[g, z])
        x_rs = zc(3, lambda d: xsend.at[g, lax.rem(z + d, 4)], lambda d: xin.at[g, d - 1])
        st = [remote(stat_in.at[g, q], stat_in.at[g, q], zsem_s.at[g, 5, d - 1], zsem_r.at[g, 5, d - 1], hd=lax.rem(q + d, 4)) for d in range(1, 4)]
        waits.extend(u_d2d + u_y + m_p + m_y + m_f + n_d2d + n_y + n_p + n_yy + n_f + [u_p, u_yy, u_f] + z_rs + z_ag + z_st + x_rs + st)

        def s1(c):
            if once('x'):
                in_copies[0].wait()
            need_weight(c)
            for j in range(4):
                o = jnp.dot(x_ref[rows, :], w1b[c, :, 2 * PAIR * j:2 * PAIR * (j + 1)], preferred_element_type=F32)
                upart[g, c, j % 2, j // 2] = o.astype(BF16)

        def sd(c):
            u_d2d[c].start()

        def s2(c):
            u_d2d[c].wait_recv()
            usend[g, c] = (upart[g, c, k, 1 - y].astype(F32) + uhalf[g, c, 1 - y].astype(F32)).astype(BF16)
            u_y[c].start()

        def s3(c):
            if once('in'):
                for cp in in_copies[1:]:
                    cp.wait()
            u_y[c].wait_recv()
            u = upart[g, c, k, y].astype(F32) + uhalf[g, c, y].astype(F32) + uin[g, c].astype(F32)
            u = (u + b1_ref[4 * c + q]).astype(BF16)
            ubuf[g, q, c] = u
            u = u.astype(F32)
            gl, _ = gelu_parts(u[:, PAIR:])
            mbuf[g, c, q] = (u[:, :PAIR] * gl).astype(BF16)
            m_y[c].start()
            m_p[c].start()
            if c == last:
                m_f[c].start()

        def s4(c):
            m_y[c].wait_recv()
            if c < last:
                m_f[c].start()

        def s5(c):
            need_weight(n_ch + c)
            m_p[c].wait_recv()
            m_f[c].wait_recv()
            blocks = [mbuf[g, c, j] for j in range(4)]
            for j in range(4):
                m_ref[4 * c + j, rows, :] = blocks[j]
            m = jnp.concatenate(blocks, axis=1)
            for n in range(0, hid, 256):
                o = jnp.dot(m, w2b[c, :, n:n + 256], preferred_element_type=F32)
                if c:
                    facc[g, :, n:n + 256] += o
                else:
                    facc[g, :, n:n + 256] = o

        def ug():
            u_yy.start()
            u_p.start()

        def uf():
            u_yy.wait_recv()
            u_f.start()

        def ud():
            u_p.wait_recv()
            u_f.wait_recv()

        def z1():
            for b in range(4):
                zsend[g, b] = facc[g, b * rz:(b + 1) * rz, :].astype(BF16)
            for d in (2, 1, 3):
                z_rs[d - 1].start()

        def z2():
            off = pl.multiple_of(z * rz, rz)
            f = facc[g, pl.ds(off, rz), :]
            for d in (1, 3, 2):
                z_rs[d - 1].wait_recv()
                f = f + zin[g, d - 1].astype(F32)
            f = f.astype(BF16)
            fsum[g, z] = f
            for d in (2, 1, 3):
                z_ag[d - 1].start()
            xoff = pl.multiple_of(row0 + z * rz, rz)
            r = ALPHA * x_ref[pl.ds(xoff, rz), :].astype(F32) + f.astype(F32) + b2_ref[...]
            gd = dy_ref[pl.ds(xoff, rz), :].astype(F32) * gam_ref[...]
            mean = jnp.sum(r, axis=1, keepdims=True) * (1.0 / hid)
            cen = r - mean
            m2 = jnp.sum(cen * cen, axis=1, keepdims=True)
            sg = jnp.sum(gd, axis=1, keepdims=True)
            sgr = jnp.sum(gd * cen, axis=1, keepdims=True)
            lane = lax.broadcasted_iota(jnp.int32, (rz, 128), 1)
            vals = jnp.where(lane == 0, mean, jnp.where(lane == 1, m2, jnp.where(lane == 2, sg, jnp.where(lane == 3, sgr, 0.0))))
            stat_in[g, q] = vals
            for s in st:
                s.start()

        def zb():
            for s in st:
                s.wait_recv()
            per = [stat_in[g, h] for h in range(4)]
            mu = sum(p[:, 0:1] for p in per) * 0.25
            m2 = sum(p[:, 1:2] + float(hid) * (p[:, 0:1] - mu) * (p[:, 0:1] - mu) for p in per)
            rho = lax.rsqrt(m2 * (1.0 / hidden) + LN_EPS)
            mg = sum(p[:, 2:3] for p in per) * (1.0 / hidden)
            mgr = rho * sum(p[:, 3:4] + (p[:, 0:1] - mu) * p[:, 2:3] for p in per) * (1.0 / hidden)
            lane = lax.broadcasted_iota(jnp.int32, (rz, 128), 1)
            tmp[:rz, :] = jnp.where(lane == 0, mu, jnp.where(lane == 1, rho, jnp.where(lane == 2, mg, jnp.where(lane == 3, mgr, 0.0))))
            stat_all[g, z] = tmp[...].T[:8, :]
            for s in z_st:
                s.start()

        def z3(d):
            if d:
                z_ag[d - 1].wait_recv()
                z_st[d - 1].wait_recv()
            src = lax.rem(z + 4 - d, 4)
            tmp[:8, :] = stat_all[g, src]
            c4 = tmp[...].T[:rz, :4]
            rr = pl.ds(pl.multiple_of(row0 + src * rz, rz), rz)
            r = ALPHA * x_ref[rr, :].astype(F32) + fsum[g, src].astype(F32) + b2_ref[...]
            dy = dy_ref[rr, :].astype(F32)
            rhat = (r - c4[:, 0:1]) * c4[:, 1:2]
            y_ref[rr, :] = (gam_ref[...] * rhat + bet_ref[...]).astype(BF16)
            dr = c4[:, 1:2] * (dy * gam_ref[...] - c4[:, 2:3] - rhat * c4[:, 3:4])
            dr_buf[rr, :] = dr
            d_ref[rr, :] = dr.astype(BF16)
            sums = (jnp.sum(dr, axis=0, keepdims=True), jnp.sum(dy * rhat, axis=0, keepdims=True), jnp.sum(dy, axis=0, keepdims=True))
            for i, s in enumerate(sums):
                if g == 0 and d == 0:
                    dsm_ref[i] = s
                else:
                    dsm_ref[i] += s

        def t1(c):
            for h in range(2):
                o = dot_nt(d_ref[rows, :], w2b[c, 256 * h:256 * (h + 1), :]).astype(BF16)
                npart[g, c, 0, h] = o[:, :PAIR]
                npart[g, c, 1, h] = o[:, PAIR:]
            n_d2d[c].start()
            if c == n_ch - 1:
                put(y_ref.at[rows, :], y_hbm.at[rows, :])
                put(d_ref.at[rows, :], d_hbm.at[rows, :])

        def t2(c):
            n_d2d[c].wait_recv()
            nsend[g, c] = (npart[g, c, k, 1 - y].astype(F32) + nhalf[g, c, 1 - y].astype(F32)).astype(BF16)
            n_y[c].start()

        def t3(c):
            n_y[c].wait_recv()
            nbuf[g, c, q] = (npart[g, c, k, y].astype(F32) + nhalf[g, c, y].astype(F32) + nin[g, c].astype(F32)).astype(BF16)
            n_yy[c].start()
            n_p[c].start()
            if c == last:
                n_f[c].start()

        def t4(c):
            n_yy[c].wait_recv()
            if c < last:
                n_f[c].start()

        def t5(c):
            n_p[c].wait_recv()
            n_f[c].wait_recv()
            parts = []
            for j in range(4):
                dm = nbuf[g, c, j].astype(F32)
                u = ubuf[g, j, c].astype(F32)
                gl, slope = gelu_parts(u[:, PAIR:])
                dv = dm * gl
                dg = dm * u[:, :PAIR] * slope
                duf = jnp.concatenate([dv, dg], axis=1)
                s = jnp.sum(duf, axis=0, keepdims=True)
                if g == 0:
                    db1_ref[4 * c + j] = s
                else:
                    db1_ref[4 * c + j] += s
                du = duf.astype(BF16)
                du_ref[4 * c + j, rows, :] = du
                parts.append(du)
            du = jnp.concatenate(parts, axis=1)
            for n in range(0, hid, 256):
                o = dot_nt(du, w1b[c, n:n + 256, :])
                if c:
                    dxacc[rows, n:n + 256] += o
                else:
                    dxacc[rows, n:n + 256] = o
            put(du_ref.at[pl.ds(4 * c, 4), rows, :], du_hbm.at[pl.ds(4 * c, 4), rows, :])

        def x1():
            put(db1_ref, db1_hbm)
            put(dsm_ref, dsm_hbm)
            for b in range(4):
                xsend[g, b] = dxacc[row0 + b * rz:row0 + (b + 1) * rz, :].astype(BF16)
            for d in (2, 1, 3):
                x_rs[d - 1].start()

        def x2():
            off = pl.multiple_of(row0 + z * rz, rz)
            t = ALPHA * dr_buf[pl.ds(off, rz), :] + dxacc[pl.ds(off, rz), :]
            for d in (1, 3, 2):
                x_rs[d - 1].wait_recv()
                t = t + xin[g, d - 1].astype(F32)
            t = t.astype(BF16)
            xown[g] = t
            for b in range(4):
                put(xown.at[g], xg_hbm.at[b])

        return dict(s1=s1, sd=sd, s2=s2, s3=s3, s4=s4, s5=s5, ug=ug, uf=uf, ud=ud, z1=z1, z2=z2, zb=zb, z3=z3, t1=t1, t2=t2, t3=t3, t4=t4, t5=t5, x1=x1, x2=x2)

    groups = {n: make_group(i) for i, n in enumerate('AB'[:GROUPS])}
    for name in order(n_ch):
        with jax.named_scope(name):
            if name == 'barrier':
                pl.semaphore_wait(bar, 6)
            elif name == 'mout':
                put(m_ref, m_hbm)
            else:
                groups[name[2]][name[:2]](*map(int, name[3:]))
    with jax.named_scope('finish'):
        for w in waits:
            w.wait_send()
        for w in outs:
            w.wait()


def order(n):
    def seq(name):
        return [f'{name}A{c}' for c in range(n)]

    o = ['s1A0', 'barrier', 'sdA0']
    for c in range(1, n):
        o += [f's1A{c}', f'sdA{c}', f's2A{c - 1}']
    o += [f's2A{n - 1}'] + seq('s3') + ['s4A0', 's4A1']
    for c in range(n):
        o += [f's5A{c}'] + ([f's4A{c + 2}'] if c + 2 < n else [])
    o += ['z1A', 'ugA', 'mout', 'z2A', 'zbA', 'z3A0', 'ufA', 'z3A1', 'z3A3', 'z3A2', 't1A0']
    for c in range(1, n):
        o += [f't1A{c}', f't2A{c - 1}']
    o += [f't2A{n - 1}', 'udA'] + seq('t3') + ['t4A0', 't4A1']
    for c in range(n):
        o += [f't5A{c}'] + ([f't4A{c + 2}'] if c + 2 < n else [])
    return o + ['x1A', 'x2A']


def grad_kernel(
    m_hbm, d_hbm, x_hbm, du_hbm, y_in, db1_in, dsm_in,
    dw1_hbm, dw2_hbm, y_hbm, db1_hbm, db2_hbm, dgam_hbm, dbet_hbm,
    m_ref, d_ref, x_ref, du_ref, y_ref, db1_ref, dsm_ref, dw1b, dw2b, isem, sem,
):
    n_blocks = m_ref.shape[0]
    hid = x_ref.shape[1]
    n_ch = n_blocks // 4
    copies = []
    loads = []

    def get(src, dst):
        cp = pltpu.make_async_copy(src, dst, isem.at[len(loads)])
        cp.start()
        loads.append(cp)

    def put(src, dst):
        cp = pltpu.make_async_copy(src, dst, sem.at[len(copies)])
        cp.start()
        copies.append(cp)

    get(d_hbm, d_ref)
    for c in range(n_ch):
        get(m_hbm.at[pl.ds(4 * c, 4)], m_ref.at[pl.ds(4 * c, 4)])
    loads[0].wait()
    for c in range(n_ch):
        loads[1 + c].wait()
        for i in range(4 * c, 4 * c + 4, 2):
            for j in range(2):
                dw2b[PAIR * (i + j):PAIR * (i + j + 1), :] = dot_tn(m_ref[i + j], d_ref[...])
            put(dw2b.at[pl.ds(PAIR * i, 2 * PAIR), :], dw2_hbm.at[pl.ds(PAIR * i, 2 * PAIR), :])
        if c == 0:
            for a, b in ((x_hbm, x_ref), (du_hbm, du_ref), (y_in, y_ref), (db1_in, db1_ref), (dsm_in, dsm_ref)):
                get(a, b)
    loads[1 + n_ch].wait()
    loads[2 + n_ch].wait()
    for i in range(0, hid, PAIR):
        for j in range(n_blocks):
            dw1b[i:i + PAIR, 2 * PAIR * j:2 * PAIR * (j + 1)] = dot_tn(x_ref[:, i:i + PAIR], du_ref[j])
        put(dw1b.at[pl.ds(i, PAIR), :], dw1_hbm.at[pl.ds(i, PAIR), :])
    for cp in loads[3 + n_ch:]:
        cp.wait()
    for a, b in ((y_ref, y_hbm), (db1_ref, db1_hbm), (dsm_ref.at[0], db2_hbm), (dsm_ref.at[1], dgam_hbm), (dsm_ref.at[2], dbet_hbm)):
        put(a, b)
    for cp in copies:
        cp.wait()


def solution(mesh):
    data_spec = P('dp', 'hd')
    hid_spec = P('hd')
    in_specs = (data_spec, P('hd', 'ff'), P('ff'), P('ff', 'hd'), hid_spec, hid_spec, hid_spec, data_spec)
    out_specs = (data_spec, data_spec, P(('dp', 'hd'), 'ff'), P(('dp', 'ff'), 'hd'), P(('dp', 'ff')), P(('dp', 'hd')), P(('dp', 'hd')), P(('dp', 'hd')))
    hbm = pl.BlockSpec(memory_space=pltpu.HBM)
    S = jax.ShapeDtypeStruct

    def device_step(x_loc, w_up, b_up, w_down, b_down, ln_gain, ln_bias, dy_loc):
        tokens, hid = x_loc.shape
        n_blocks = w_up.shape[1] // (2 * PAIR)
        n_ch = n_blocks // 4
        tn = tokens // GROUPS
        g = GROUPS
        rz = tn // 4
        V = pltpu.VMEM
        dma = pltpu.SemaphoreType.DMA
        outs = pl.pallas_call(
            main_kernel,
            out_shape=(
                S((tokens, hid), BF16), S((n_blocks, tokens, PAIR), BF16), S((tokens, hid), BF16), S((n_blocks, tokens, 2 * PAIR), BF16),
                S((4, rz, hid), BF16), S((n_blocks, 1, 2 * PAIR), F32), S((3, 1, hid), F32),
            ),
            in_specs=[hbm] * 8,
            out_specs=[hbm] * 7,
            scratch_shapes=[
                V((tokens, hid), BF16), V((n_blocks, tokens, PAIR), BF16), V((tokens, hid), BF16), V((n_blocks, tokens, 2 * PAIR), BF16),
                V((n_blocks, 1, 2 * PAIR), F32), V((3, 1, hid), F32),
                V((tokens, hid), BF16), V((tokens, hid), BF16), V((n_blocks, 1, 2 * PAIR), F32), V((1, hid), F32), V((1, hid), F32), V((1, hid), F32),
                V((n_ch, hid, 8 * PAIR), BF16), V((n_ch, 4 * PAIR, hid), BF16),
                V((g, n_ch, 2, 2, tn, 2 * PAIR), BF16), V((g, n_ch, 2, tn, 2 * PAIR), BF16), V((g, n_ch, tn, 2 * PAIR), BF16), V((g, n_ch, tn, 2 * PAIR), BF16),
                V((g, 4, n_ch, tn, 2 * PAIR), BF16), V((g, n_ch, 4, tn, PAIR), BF16),
                V((g, tn, hid), F32), V((g, 4, rz, hid), BF16), V((g, 3, rz, hid), BF16), V((g, 4, rz, hid), BF16),
                V((g, 4, rz, 128), F32), V((g, 4, 8, 128), F32), V((128, 128), F32), V((tokens, hid), F32),
                V((g, n_ch, 2, 2, tn, PAIR), BF16), V((g, n_ch, 2, tn, PAIR), BF16), V((g, n_ch, tn, PAIR), BF16), V((g, n_ch, tn, PAIR), BF16),
                V((g, n_ch, 4, tn, PAIR), BF16), V((tokens, hid), F32),
                V((g, 4, rz, hid), BF16), V((g, 3, rz, hid), BF16), V((g, rz, hid), BF16),
                dma((2 * n_ch,)), dma((6,)), dma(((2 + n_ch) * g + 7,)), dma((g, 10, n_ch)), dma((g, 10, n_ch)), dma((g, 3)), dma((g, 3)), dma((g, 6, 3)), dma((g, 6, 3)),
            ],
            compiler_params=pltpu.CompilerParams(collective_id=0, has_side_effects=True, vmem_limit_bytes=VMEM_LIMIT),
            name='mlp_main',
        )(x_loc, w_up, b_up.reshape(n_blocks, 1, 2 * PAIR), w_down, b_down.reshape(1, hid), ln_gain.reshape(1, hid), ln_bias.reshape(1, hid), dy_loc)
        y_a, m_a, d_a, du_a, xg, db1, dsm = outs
        dx = lax.all_to_all(xg, 'ff', 0, 0)
        vec = S((1, hid), F32)
        dw_up, dw_down, y_o, db1_o, db2_o, dg_o, dbt_o = pl.pallas_call(
            grad_kernel,
            out_shape=(S((hid, n_blocks * 2 * PAIR), F32), S((n_blocks * PAIR, hid), F32), S(y_a.shape, BF16), S(db1.shape, F32), vec, vec, vec),
            in_specs=[hbm] * 7,
            out_specs=[hbm] * 7,
            scratch_shapes=[
                V((n_blocks, tokens, PAIR), BF16), V((tokens, hid), BF16), V((tokens, hid), BF16), V((n_blocks, tokens, 2 * PAIR), BF16),
                V((tokens, hid), BF16), V((n_blocks, 1, 2 * PAIR), F32), V((3, 1, hid), F32),
                V((hid, n_blocks * 2 * PAIR), F32), V((n_blocks * PAIR, hid), F32), dma((6 + n_ch,)), dma((n_blocks // 2 + hid // PAIR + 5,)),
            ],
            compiler_params=pltpu.CompilerParams(vmem_limit_bytes=VMEM_LIMIT),
            cost_estimate=pl.CostEstimate(flops=10**10, bytes_accessed=10**7, transcendentals=0),
            name='mlp_grads',
        )(m_a, d_a, x_loc, du_a, y_a, db1, dsm)
        return (y_o, dx.reshape(tokens, hid), dw_up, dw_down, db1_o.reshape(-1), db2_o.reshape(-1), dg_o.reshape(-1), dbt_o.reshape(-1))

    return jax.shard_map(device_step, mesh=mesh, in_specs=in_specs, out_specs=out_specs, check_vma=False)
```

```python
import functools
import math

import jax
import jax.numpy as jnp
from jax import lax
from jax.experimental import pallas as pl
from jax.experimental.pallas import tpu as pltpu
from jax.sharding import PartitionSpec as P

PAIR = 128
ALPHA = math.sqrt(140.0)
LN_EPS = 1e-5
GELU_K = math.sqrt(2.0 / math.pi)
GELU_C = 0.044715
MESH = pl.DeviceIdType.MESH
F32 = jnp.float32
BF16 = jnp.bfloat16

GROUPS = 1
VMEM_LIMIT = 60 * 2**20
LOOKAHEAD = 3


def gelu_parts(z):
    t = jnp.tanh(GELU_K * (z + GELU_C * (z * z * z)))
    cdf = 0.5 * (1.0 + t)
    slope = cdf + z * (0.5 * (1.0 - t * t) * (GELU_K * (1.0 + (3.0 * GELU_C) * (z * z))))
    return z * cdf, slope


def dot_nt(a, b):
    return lax.dot_general(a, b, (((1,), (1,)), ((), ())), preferred_element_type=F32)


def dot_tn(a, b):
    return lax.dot_general(a, b, (((0,), (0,)), ((), ())), preferred_element_type=F32)


def main_kernel(
    x_hbm, w1_hbm, b1_hbm, w2_hbm, b2_hbm, gam_hbm, bet_hbm, dy_hbm,
    y_hbm, m_hbm, d_hbm, du_hbm, xg_hbm, db1_hbm, dsm_hbm,
    y_ref, m_ref, d_ref, du_ref, db1_ref, dsm_ref,
    x_ref, dy_ref, b1_ref, b2_ref, gam_ref, bet_ref,
    w1b, w2b, upart, uhalf, usend, uin, ubuf, mbuf, facc, zsend, zin, fsum, stat_in, stat_all, tmp, dr_buf,
    npart, nhalf, nsend, nin, nbuf, dxacc, xsend, xin, xown,
    wsem, isem, osem, chunk_s, chunk_r, full_s, full_r, zsem_s, zsem_r,
):
    n_ch = w1b.shape[0]
    tokens, hid = x_ref.shape
    hidden = 4 * hid
    tn = tokens // GROUPS
    rz = tn // 4
    cw = 8 * PAIR
    q = lax.axis_index('hd')
    z = lax.axis_index('ff')
    k = lax.rem(q, 2)
    y = lax.div(q, 2)
    pq = q + 1 - 2 * k
    yq = lax.rem(q + 2, 4)
    dq = lax.rem(pq + 2, 4)
    pair, place = lax.div(z, 2), lax.rem(z, 2)
    inner = pair + place - 2 * pair * place
    d_a, d_b = 3 - 2 * pair, 1 + 2 * pair
    last = n_ch - 1

    def remote(src, dst, ss, rs, **dev):
        return pltpu.make_async_remote_copy(src_ref=src, dst_ref=dst, send_sem=ss, recv_sem=rs, device_id=dev, device_id_type=MESH)

    w_copies = [pltpu.make_async_copy(w1_hbm.at[:, pl.ds(cw * c, cw)], w1b.at[c], wsem.at[c]) for c in range(n_ch)]
    w_copies += [pltpu.make_async_copy(w2_hbm.at[pl.ds(4 * PAIR * c, 4 * PAIR), :], w2b.at[c], wsem.at[n_ch + c]) for c in range(n_ch)]
    in_copies = [pltpu.make_async_copy(a, b, isem.at[i]) for i, (a, b) in enumerate(((x_hbm, x_ref), (b1_hbm, b1_ref), (dy_hbm, dy_ref), (b2_hbm, b2_ref), (gam_hbm, gam_ref), (bet_hbm, bet_ref)))]
    started = [0]
    landed = set()

    def need_weight(i):
        while started[0] < min(i + LOOKAHEAD, 2 * n_ch):
            w_copies[started[0]].start()
            started[0] += 1
        if i not in landed:
            landed.add(i)
            w_copies[i].wait()

    bar = pltpu.get_barrier_semaphore()
    for d in range(1, 4):
        pl.semaphore_signal(bar, inc=1, device_id={'ff': lax.rem(z + d, 4)}, device_id_type=MESH)
    for d in range(1, 4):
        pl.semaphore_signal(bar, inc=1, device_id={'hd': lax.rem(q + d, 4)}, device_id_type=MESH)
    in_copies[0].start()
    for i in range(LOOKAHEAD):
        w_copies[i].start()
    started[0] = LOOKAHEAD
    for cp in in_copies[1:]:
        cp.start()

    tmp[...] = jnp.zeros_like(tmp)
    waits = []
    outs = []

    def put(src, dst):
        cp = pltpu.make_async_copy(src, dst, osem.at[len(outs)])
        cp.start()
        outs.append(cp)

    seen = set()

    def once(name):
        new = name not in seen
        seen.add(name)
        return new

    def make_group(g):
        row0 = g * tn
        rows = pl.ds(row0, tn)

        def ch(kind, c):
            return chunk_s.at[g, kind, c], chunk_r.at[g, kind, c]

        u_d2d = [remote(upart.at[g, c, 1 - k], uhalf.at[g, c], *ch(0, c), hd=pq) for c in range(n_ch)]
        u_y = [remote(usend.at[g, c], uin.at[g, c], *ch(1, c), hd=yq) for c in range(n_ch)]
        m_p = [remote(mbuf.at[g, c, q], mbuf.at[g, c, q], *ch(2, c), hd=pq) for c in range(n_ch)]
        m_y = [remote(mbuf.at[g, c, q], mbuf.at[g, c, q], *ch(3, c), hd=yq) for c in range(n_ch)]
        m_f = [remote(mbuf.at[g, c, yq], mbuf.at[g, c, yq], *ch(4, c), hd=pq) for c in range(last)]
        m_f.append(remote(mbuf.at[g, last, q], mbuf.at[g, last, q], *ch(4, last), hd=dq))
        n_d2d = [remote(npart.at[g, c, 1 - k], nhalf.at[g, c], *ch(5, c), hd=pq) for c in range(n_ch)]
        n_y = [remote(nsend.at[g, c], nin.at[g, c], *ch(6, c), hd=yq) for c in range(n_ch)]
        n_p = [remote(nbuf.at[g, c, q], nbuf.at[g, c, q], *ch(7, c), hd=pq) for c in range(n_ch)]
        n_yy = [remote(nbuf.at[g, c, q], nbuf.at[g, c, q], *ch(8, c), hd=yq) for c in range(n_ch)]
        n_f = [remote(nbuf.at[g, c, yq], nbuf.at[g, c, yq], *ch(9, c), hd=pq) for c in range(last)]
        n_f.append(remote(nbuf.at[g, last, q], nbuf.at[g, last, q], *ch(9, last), hd=dq))
        u_p = remote(ubuf.at[g, q], ubuf.at[g, q], full_s.at[g, 0], full_r.at[g, 0], hd=pq)
        u_yy = remote(ubuf.at[g, q], ubuf.at[g, q], full_s.at[g, 1], full_r.at[g, 1], hd=yq)
        u_f = remote(ubuf.at[g, yq], ubuf.at[g, yq], full_s.at[g, 2], full_r.at[g, 2], hd=pq)

        def zc(kind, src, dst):
            return [remote(src(d), dst(d), zsem_s.at[g, kind, d - 1], zsem_r.at[g, kind, d - 1], ff=lax.rem(z + d, 4)) for d in range(1, 4)]

        z_rs = zc(0, lambda d: zsend.at[g, lax.rem(z + d, 4)], lambda d: zin.at[g, d - 1])
        def gather(d, block, dev):
            return remote(fsum.at[g, block], fsum.at[g, block], zsem_s.at[g, 1, d - 1], zsem_r.at[g, 1, d - 1], ff=dev)

        z_ag = [gather(d_a, z, lax.rem(z + d_a, 4)), gather(2, z + inner * (3 - 2 * z), (1 - inner) * lax.rem(z + 2, 4) + inner * (z + 1 - 2 * place)), gather(d_b, z, lax.rem(z + d_b, 4))]
        z_sd = [remote(stat_all.at[g, z], stat_all.at[g, z], zsem_s.at[g, 2, d - 1], zsem_r.at[g, 2, d - 1], ff=lax.rem(z + d, 4)) for d in (d_a, 2, d_b)]
        z_st = zc(2, lambda d: stat_all.at[g, z], lambda d: stat_all.at[g, z])
        z_out = [remote(zsend.at[g, lax.rem(z + d, 4)], zin.at[g, d - 1], zsem_s.at[g, 0, d - 1], zsem_r.at[g, 0, d - 1], ff=lax.rem(z + d, 4)) for d in (d_a, 2, d_b)]
        x_out = [remote(xsend.at[g, lax.rem(z + d, 4)], xin.at[g, d - 1], zsem_s.at[g, 3, d - 1], zsem_r.at[g, 3, d - 1], ff=lax.rem(z + d, 4)) for d in (d_a, 2, d_b)]
        x_rs = zc(3, lambda d: xsend.at[g, lax.rem(z + d, 4)], lambda d: xin.at[g, d - 1])
        st = [remote(stat_in.at[g, q], stat_in.at[g, q], zsem_s.at[g, 5, d - 1], zsem_r.at[g, 5, d - 1], hd=lax.rem(q + d, 4)) for d in range(1, 4)]
        waits.extend(u_d2d + u_y + m_p + m_y + m_f + n_d2d + n_y + n_p + n_yy + n_f + [u_p, u_yy, u_f] + z_rs + z_ag + z_st + x_rs + st)

        def s1(c):
            if once('x'):
                in_copies[0].wait()
            need_weight(c)
            for j in range(4):
                o = jnp.dot(x_ref[rows, :], w1b[c, :, 2 * PAIR * j:2 * PAIR * (j + 1)], preferred_element_type=F32)
                upart[g, c, j % 2, j // 2] = o.astype(BF16)

        def sd(c):
            u_d2d[c].start()

        def s2(c):
            u_d2d[c].wait_recv()
            usend[g, c] = (upart[g, c, k, 1 - y].astype(F32) + uhalf[g, c, 1 - y].astype(F32)).astype(BF16)
            u_y[c].start()

        def s3(c):
            if once('in'):
                for cp in in_copies[1:]:
                    cp.wait()
            u_y[c].wait_recv()
            u = upart[g, c, k, y].astype(F32) + uhalf[g, c, y].astype(F32) + uin[g, c].astype(F32)
            u = (u + b1_ref[4 * c + q]).astype(BF16)
            ubuf[g, q, c] = u
            u = u.astype(F32)
            gl, _ = gelu_parts(u[:, PAIR:])
            mbuf[g, c, q] = (u[:, :PAIR] * gl).astype(BF16)
            m_y[c].start()
            m_p[c].start()
            if c == last:
                m_f[c].start()

        def s4(c):
            m_y[c].wait_recv()
            if c < last:
                m_f[c].start()

        def s5(c):
            need_weight(n_ch + c)
            m_p[c].wait_recv()
            m_f[c].wait_recv()
            blocks = [mbuf[g, c, j] for j in range(4)]
            for j in range(4):
                m_ref[4 * c + j, rows, :] = blocks[j]
            m = jnp.concatenate(blocks, axis=1)
            for n in range(0, hid, 256):
                o = jnp.dot(m, w2b[c, :, n:n + 256], preferred_element_type=F32)
                if c:
                    facc[g, :, n:n + 256] += o
                else:
                    facc[g, :, n:n + 256] = o

        def ug():
            u_yy.start()
            u_p.start()

        def uf():
            u_yy.wait_recv()
            u_f.start()

        def ud():
            u_p.wait_recv()
            u_f.wait_recv()

        def z1():
            for b in range(4):
                zsend[g, b] = facc[g, b * rz:(b + 1) * rz, :].astype(BF16)
            for cp in z_out:
                cp.start()

        def z2():
            off = pl.multiple_of(z * rz, rz)
            f = facc[g, pl.ds(off, rz), :]
            for d in (1, 3, 2):
                z_rs[d - 1].wait_recv()
                f = f + zin[g, d - 1].astype(F32)
            f = f.astype(BF16)
            fsum[g, z] = f
            z_ag[2].start()
            z_ag[0].start()
            pl.when(inner == 0)(z_ag[1].start)
            xoff = pl.multiple_of(row0 + z * rz, rz)
            r = ALPHA * x_ref[pl.ds(xoff, rz), :].astype(F32) + f.astype(F32) + b2_ref[...]
            gd = dy_ref[pl.ds(xoff, rz), :].astype(F32) * gam_ref[...]
            mean = jnp.sum(r, axis=1, keepdims=True) * (1.0 / hid)
            cen = r - mean
            m2 = jnp.sum(cen * cen, axis=1, keepdims=True)
            sg = jnp.sum(gd, axis=1, keepdims=True)
            sgr = jnp.sum(gd * cen, axis=1, keepdims=True)
            lane = lax.broadcasted_iota(jnp.int32, (rz, 128), 1)
            vals = jnp.where(lane == 0, mean, jnp.where(lane == 1, m2, jnp.where(lane == 2, sg, jnp.where(lane == 3, sgr, 0.0))))
            stat_in[g, q] = vals
            for s in st:
                s.start()

        def zb():
            for s in st:
                s.wait_recv()
            per = [stat_in[g, h] for h in range(4)]
            mu = sum(p[:, 0:1] for p in per) * 0.25
            m2 = sum(p[:, 1:2] + float(hid) * (p[:, 0:1] - mu) * (p[:, 0:1] - mu) for p in per)
            rho = lax.rsqrt(m2 * (1.0 / hidden) + LN_EPS)
            mg = sum(p[:, 2:3] for p in per) * (1.0 / hidden)
            mgr = rho * sum(p[:, 3:4] + (p[:, 0:1] - mu) * p[:, 2:3] for p in per) * (1.0 / hidden)
            lane = lax.broadcasted_iota(jnp.int32, (rz, 128), 1)
            tmp[:rz, :] = jnp.where(lane == 0, mu, jnp.where(lane == 1, rho, jnp.where(lane == 2, mg, jnp.where(lane == 3, mgr, 0.0))))
            stat_all[g, z] = tmp[...].T[:8, :]
            for s in z_st:
                s.start()

        def z3(i):
            d = (0, d_a, d_b, 2)[i]
            if i:
                e = (0, 2, 1)[i - 1]
                z_ag[e].wait_recv()
                if i == 1:
                    pl.when(inner == 1)(z_ag[1].start)
                z_sd[e].wait_recv()
            src = lax.rem(z + 4 - d, 4)
            tmp[:8, :] = stat_all[g, src]
            c4 = tmp[...].T[:rz, :4]
            rr = pl.ds(pl.multiple_of(row0 + src * rz, rz), rz)
            r = ALPHA * x_ref[rr, :].astype(F32) + fsum[g, src].astype(F32) + b2_ref[...]
            dy = dy_ref[rr, :].astype(F32)
            rhat = (r - c4[:, 0:1]) * c4[:, 1:2]
            y_ref[rr, :] = (gam_ref[...] * rhat + bet_ref[...]).astype(BF16)
            dr = c4[:, 1:2] * (dy * gam_ref[...] - c4[:, 2:3] - rhat * c4[:, 3:4])
            dr_buf[rr, :] = dr
            d_ref[rr, :] = dr.astype(BF16)
            sums = (jnp.sum(dr, axis=0, keepdims=True), jnp.sum(dy * rhat, axis=0, keepdims=True), jnp.sum(dy, axis=0, keepdims=True))
            for e, s in enumerate(sums):
                if g == 0 and i == 0:
                    dsm_ref[e] = s
                else:
                    dsm_ref[e] += s

        def t1(c):
            for h in range(2):
                o = dot_nt(d_ref[rows, :], w2b[c, 256 * h:256 * (h + 1), :]).astype(BF16)
                npart[g, c, 0, h] = o[:, :PAIR]
                npart[g, c, 1, h] = o[:, PAIR:]
            n_d2d[c].start()
            if c == n_ch - 1:
                put(y_ref.at[rows, :], y_hbm.at[rows, :])
                put(d_ref.at[rows, :], d_hbm.at[rows, :])

        def t2(c):
            n_d2d[c].wait_recv()
            nsend[g, c] = (npart[g, c, k, 1 - y].astype(F32) + nhalf[g, c, 1 - y].astype(F32)).astype(BF16)
            n_y[c].start()

        def t3(c):
            n_y[c].wait_recv()
            nbuf[g, c, q] = (npart[g, c, k, y].astype(F32) + nhalf[g, c, y].astype(F32) + nin[g, c].astype(F32)).astype(BF16)
            n_yy[c].start()
            n_p[c].start()
            if c == last:
                n_f[c].start()

        def t4(c):
            n_yy[c].wait_recv()
            if c < last:
                n_f[c].start()

        def t5(c):
            n_p[c].wait_recv()
            n_f[c].wait_recv()
            parts = []
            for j in range(4):
                dm = nbuf[g, c, j].astype(F32)
                u = ubuf[g, j, c].astype(F32)
                gl, slope = gelu_parts(u[:, PAIR:])
                dv = dm * gl
                dg = dm * u[:, :PAIR] * slope
                duf = jnp.concatenate([dv, dg], axis=1)
                s = jnp.sum(duf, axis=0, keepdims=True)
                if g == 0:
                    db1_ref[4 * c + j] = s
                else:
                    db1_ref[4 * c + j] += s
                du = duf.astype(BF16)
                du_ref[4 * c + j, rows, :] = du
                parts.append(du)
            du = jnp.concatenate(parts, axis=1)
            for n in range(0, hid, 256):
                o = dot_nt(du, w1b[c, n:n + 256, :])
                if c:
                    dxacc[rows, n:n + 256] += o
                else:
                    dxacc[rows, n:n + 256] = o
            put(du_ref.at[pl.ds(4 * c, 4), rows, :], du_hbm.at[pl.ds(4 * c, 4), rows, :])

        def x1():
            put(db1_ref, db1_hbm)
            put(dsm_ref, dsm_hbm)
            for b in range(4):
                xsend[g, b] = dxacc[row0 + b * rz:row0 + (b + 1) * rz, :].astype(BF16)
            for cp in x_out:
                cp.start()

        def x2():
            off = pl.multiple_of(row0 + z * rz, rz)
            t = ALPHA * dr_buf[pl.ds(off, rz), :] + dxacc[pl.ds(off, rz), :]
            for d in (1, 3, 2):
                x_rs[d - 1].wait_recv()
                t = t + xin[g, d - 1].astype(F32)
            t = t.astype(BF16)
            xown[g] = t
            for b in range(4):
                put(xown.at[g], xg_hbm.at[b])

        return dict(s1=s1, sd=sd, s2=s2, s3=s3, s4=s4, s5=s5, ug=ug, uf=uf, ud=ud, z1=z1, z2=z2, zb=zb, z3=z3, t1=t1, t2=t2, t3=t3, t4=t4, t5=t5, x1=x1, x2=x2)

    groups = {n: make_group(i) for i, n in enumerate('AB'[:GROUPS])}
    for name in order(n_ch):
        with jax.named_scope(name):
            if name == 'barrier':
                pl.semaphore_wait(bar, 6)
            elif name == 'mout':
                put(m_ref, m_hbm)
            else:
                groups[name[2]][name[:2]](*map(int, name[3:]))
    with jax.named_scope('finish'):
        for w in waits:
            w.wait_send()
        for w in outs:
            w.wait()


def order(n):
    def seq(name):
        return [f'{name}A{c}' for c in range(n)]

    o = ['s1A0', 'barrier', 'sdA0']
    for c in range(1, n):
        o += [f's1A{c}', f'sdA{c}', f's2A{c - 1}']
    o += [f's2A{n - 1}'] + seq('s3') + ['s4A0', 's4A1']
    for c in range(n):
        o += [f's5A{c}'] + ([f's4A{c + 2}'] if c + 2 < n else [])
    o += ['z1A', 'ugA', 'mout', 'z2A', 'zbA', 'z3A0', 'ufA', 'z3A1', 'z3A2', 'z3A3', 't1A0']
    for c in range(1, n):
        o += [f't1A{c}', f't2A{c - 1}']
    o += [f't2A{n - 1}', 'udA'] + seq('t3') + ['t4A0', 't4A1']
    for c in range(n):
        o += [f't5A{c}'] + ([f't4A{c + 2}'] if c + 2 < n else [])
    return o + ['x1A', 'x2A']


def grad_kernel(
    m_hbm, d_hbm, x_hbm, du_hbm, y_in, db1_in, dsm_in,
    dw1_hbm, dw2_hbm, y_hbm, db1_hbm, db2_hbm, dgam_hbm, dbet_hbm,
    m_ref, d_ref, x_ref, du_ref, y_ref, db1_ref, dsm_ref, dw1b, dw2b, isem, sem,
):
    n_blocks = m_ref.shape[0]
    hid = x_ref.shape[1]
    n_ch = n_blocks // 4
    copies = []
    loads = []

    def get(src, dst):
        cp = pltpu.make_async_copy(src, dst, isem.at[len(loads)])
        cp.start()
        loads.append(cp)

    def put(src, dst):
        cp = pltpu.make_async_copy(src, dst, sem.at[len(copies)])
        cp.start()
        copies.append(cp)

    get(d_hbm, d_ref)
    for c in range(n_ch):
        get(m_hbm.at[pl.ds(4 * c, 4)], m_ref.at[pl.ds(4 * c, 4)])
    loads[0].wait()
    for c in range(n_ch):
        loads[1 + c].wait()
        for i in range(4 * c, 4 * c + 4, 2):
            for j in range(2):
                dw2b[PAIR * (i + j):PAIR * (i + j + 1), :] = dot_tn(m_ref[i + j], d_ref[...])
            put(dw2b.at[pl.ds(PAIR * i, 2 * PAIR), :], dw2_hbm.at[pl.ds(PAIR * i, 2 * PAIR), :])
        if c == 0:
            for a, b in ((x_hbm, x_ref), (du_hbm, du_ref), (y_in, y_ref), (db1_in, db1_ref), (dsm_in, dsm_ref)):
                get(a, b)
    loads[1 + n_ch].wait()
    loads[2 + n_ch].wait()
    for i in range(0, hid, PAIR):
        for j in range(n_blocks):
            dw1b[i:i + PAIR, 2 * PAIR * j:2 * PAIR * (j + 1)] = dot_tn(x_ref[:, i:i + PAIR], du_ref[j])
        put(dw1b.at[pl.ds(i, PAIR), :], dw1_hbm.at[pl.ds(i, PAIR), :])
    for cp in loads[3 + n_ch:]:
        cp.wait()
    for a, b in ((y_ref, y_hbm), (db1_ref, db1_hbm), (dsm_ref.at[0], db2_hbm), (dsm_ref.at[1], dgam_hbm), (dsm_ref.at[2], dbet_hbm)):
        put(a, b)
    for cp in copies:
        cp.wait()


def solution(mesh):
    data_spec = P('dp', 'hd')
    hid_spec = P('hd')
    in_specs = (data_spec, P('hd', 'ff'), P('ff'), P('ff', 'hd'), hid_spec, hid_spec, hid_spec, data_spec)
    out_specs = (data_spec, data_spec, P(('dp', 'hd'), 'ff'), P(('dp', 'ff'), 'hd'), P(('dp', 'ff')), P(('dp', 'hd')), P(('dp', 'hd')), P(('dp', 'hd')))
    hbm = pl.BlockSpec(memory_space=pltpu.HBM)
    S = jax.ShapeDtypeStruct

    def device_step(x_loc, w_up, b_up, w_down, b_down, ln_gain, ln_bias, dy_loc):
        tokens, hid = x_loc.shape
        n_blocks = w_up.shape[1] // (2 * PAIR)
        n_ch = n_blocks // 4
        tn = tokens // GROUPS
        g = GROUPS
        rz = tn // 4
        V = pltpu.VMEM
        dma = pltpu.SemaphoreType.DMA
        outs = pl.pallas_call(
            main_kernel,
            out_shape=(
                S((tokens, hid), BF16), S((n_blocks, tokens, PAIR), BF16), S((tokens, hid), BF16), S((n_blocks, tokens, 2 * PAIR), BF16),
                S((4, rz, hid), BF16), S((n_blocks, 1, 2 * PAIR), F32), S((3, 1, hid), F32),
            ),
            in_specs=[hbm] * 8,
            out_specs=[hbm] * 7,
            scratch_shapes=[
                V((tokens, hid), BF16), V((n_blocks, tokens, PAIR), BF16), V((tokens, hid), BF16), V((n_blocks, tokens, 2 * PAIR), BF16),
                V((n_blocks, 1, 2 * PAIR), F32), V((3, 1, hid), F32),
                V((tokens, hid), BF16), V((tokens, hid), BF16), V((n_blocks, 1, 2 * PAIR), F32), V((1, hid), F32), V((1, hid), F32), V((1, hid), F32),
                V((n_ch, hid, 8 * PAIR), BF16), V((n_ch, 4 * PAIR, hid), BF16),
                V((g, n_ch, 2, 2, tn, 2 * PAIR), BF16), V((g, n_ch, 2, tn, 2 * PAIR), BF16), V((g, n_ch, tn, 2 * PAIR), BF16), V((g, n_ch, tn, 2 * PAIR), BF16),
                V((g, 4, n_ch, tn, 2 * PAIR), BF16), V((g, n_ch, 4, tn, PAIR), BF16),
                V((g, tn, hid), F32), V((g, 4, rz, hid), BF16), V((g, 3, rz, hid), BF16), V((g, 4, rz, hid), BF16),
                V((g, 4, rz, 128), F32), V((g, 4, 8, 128), F32), V((128, 128), F32), V((tokens, hid), F32),
                V((g, n_ch, 2, 2, tn, PAIR), BF16), V((g, n_ch, 2, tn, PAIR), BF16), V((g, n_ch, tn, PAIR), BF16), V((g, n_ch, tn, PAIR), BF16),
                V((g, n_ch, 4, tn, PAIR), BF16), V((tokens, hid), F32),
                V((g, 4, rz, hid), BF16), V((g, 3, rz, hid), BF16), V((g, rz, hid), BF16),
                dma((2 * n_ch,)), dma((6,)), dma(((2 + n_ch) * g + 7,)), dma((g, 10, n_ch)), dma((g, 10, n_ch)), dma((g, 3)), dma((g, 3)), dma((g, 6, 3)), dma((g, 6, 3)),
            ],
            compiler_params=pltpu.CompilerParams(collective_id=0, has_side_effects=True, vmem_limit_bytes=VMEM_LIMIT),
            name='mlp_main',
        )(x_loc, w_up, b_up.reshape(n_blocks, 1, 2 * PAIR), w_down, b_down.reshape(1, hid), ln_gain.reshape(1, hid), ln_bias.reshape(1, hid), dy_loc)
        y_a, m_a, d_a, du_a, xg, db1, dsm = outs
        dx = lax.all_to_all(xg, 'ff', 0, 0)
        vec = S((1, hid), F32)
        dw_up, dw_down, y_o, db1_o, db2_o, dg_o, dbt_o = pl.pallas_call(
            grad_kernel,
            out_shape=(S((hid, n_blocks * 2 * PAIR), F32), S((n_blocks * PAIR, hid), F32), S(y_a.shape, BF16), S(db1.shape, F32), vec, vec, vec),
            in_specs=[hbm] * 7,
            out_specs=[hbm] * 7,
            scratch_shapes=[
                V((n_blocks, tokens, PAIR), BF16), V((tokens, hid), BF16), V((tokens, hid), BF16), V((n_blocks, tokens, 2 * PAIR), BF16),
                V((tokens, hid), BF16), V((n_blocks, 1, 2 * PAIR), F32), V((3, 1, hid), F32),
                V((hid, n_blocks * 2 * PAIR), F32), V((n_blocks * PAIR, hid), F32), dma((6 + n_ch,)), dma((n_blocks // 2 + hid // PAIR + 5,)),
            ],
            compiler_params=pltpu.CompilerParams(vmem_limit_bytes=VMEM_LIMIT),
            cost_estimate=pl.CostEstimate(flops=10**10, bytes_accessed=10**7, transcendentals=0),
            name='mlp_grads',
        )(m_a, d_a, x_loc, du_a, y_a, db1, dsm)
        return (y_o, dx.reshape(tokens, hid), dw_up, dw_down, db1_o.reshape(-1), db2_o.reshape(-1), dg_o.reshape(-1), dbt_o.reshape(-1))

    return jax.shard_map(device_step, mesh=mesh, in_specs=in_specs, out_specs=out_specs, check_vma=False)
```
